32 devices in a mesh: sfc: 16 (over z, y, x), grp: 2 (over core).
Axes of the slice: x: 2, y: 2, z: 4, core: 2. Of those that a mesh axis runs over, the one named last changes fastest.
Arguments:
- right_side: float32 [5, 5, 5, 4096], P(None, None, None, ('sfc', 'grp')), may hold values from -8 to 8
- cell_level: int32 [4096], P(('sfc', 'grp')), may hold values from 0 to 3
- own_slot: int32 [12288], P(('sfc', 'grp')), may hold values from 0 to 767
- near_slot: int32 [12288], P(('sfc', 'grp')), may hold values from 0 to 1151, as said below
- face_kind: int32 [12288], P(('sfc', 'grp')), may hold values from 0 to 5
- orientation: int32 [12288], P(('sfc', 'grp')), may hold values from 0 to 7
- penalty: float32 [12288], P(('sfc', 'grp')), may hold values from 2 to 32
- send_slots: int32 [12288], P(('sfc', 'grp')), may hold values from 0 to 767
- subface_maps: float32 [4, 25, 25], replicated, may hold values from -1.25 to 1.25
Outputs:
- solution: float32 [5, 5, 5, 4096], P(None, None, None, ('sfc', 'grp'))
- residual: float32 [5, 5, 5, 4096], P(None, None, None, ('sfc', 'grp'))
The draws below stay inside these ranges and needn't reach their ends.
Inputs may be any that keep to these rules, and one draw needn't show every extreme that they name: `own_slot`: a face slot f * 128 + c of the same device. `near_slot`: 768 + k * 96 + i for position i of the received block k; since a device has exactly 384 entries, its near slots are a permutation of its 384 received positions. `face_kind`: 0 boundary face, 1 conforming face, 2 + s the fine side of a hanging face with subface s. `send_slots`: a device's entries k * 96 to k * 96 + 95 are face slots of its own cells sent to the device at offset (+1, -1, +2, -2)[k].
All inputs are finite; a program needn't handle non-finite values.
Results may differ from the reference program's by a relative error of at most 0.00021.
Values sent between devices are 32-bit elements; how exact they have to be, the bound alone decides.
A program may use at most 64 MiB of HBM per device.

```python
import math
import jax
import jax.numpy as jnp
import numpy as np
from jax import lax

NODES = 5
CELLS_DEV = 128
GHOST = 96
ITERS = 3
ENTRY_DEV = 384
CELLS = 4096
ENTRIES = 12288
SENDS = 12288
N_SFC = 16
N_GRP = 2


def draw_right_side(key, part):
    position = jnp.arange(CELLS, dtype=jnp.float32) / CELLS
    values = jax.random.normal(key, (NODES, NODES, NODES, CELLS), jnp.float32)
    return jnp.clip(values, -4.0, 4.0) * jnp.sqrt(1.0 + 2.0 * position)


def draw_near_slot(key, part):
    devices = ENTRIES // ENTRY_DEV
    received = 4 * GHOST
    local_key = jax.random.fold_in(key, 11)
    order_key = jax.random.fold_in(key, 23)
    local = jax.random.randint(local_key, (devices, ENTRY_DEV), 0, 6 * CELLS_DEV, dtype=jnp.int32)
    device_keys = jax.random.split(order_key, devices)
    order = jax.vmap(lambda single: jax.random.permutation(single, ENTRY_DEV))(device_keys).astype(jnp.int32)
    chosen = jnp.where(order < received, 6 * CELLS_DEV + order, local)
    return chosen.reshape(-1).astype(jnp.int32)


def place_ends(drawn, stream_key, smallest, largest):
    longest = drawn.shape.index(max(drawn.shape))
    spots = []
    for shift in (0, 1):
        where = [jax.random.randint(jax.random.fold_in(stream_key, axis), (), 0, length) for axis, length in enumerate(drawn.shape)]
        where[longest] = (where[longest] + shift) % drawn.shape[longest]
        spots.append(tuple(where))
    return drawn.at[spots[0]].set(smallest).at[spots[1]].set(largest)


def block_levels(own_key, shape, cuts, least, largest):
    loudness, own = 1.0, jax.random.fold_in(own_key, 6)
    for dim, blocks in cuts:
        heights = jnp.exp(jax.random.uniform(jax.random.fold_in(own, dim), (blocks,), jnp.float32, least / len(cuts), largest / len(cuts)))
        loudness = loudness * jnp.repeat(heights, shape[dim] // blocks).reshape([-1 if axis == dim else 1 for axis in range(len(shape))])
    return loudness


def centred(rng, shape, scale, reach, kind=jnp.bfloat16):
    values = jax.random.normal(rng, shape, jnp.float32) * scale
    return jnp.minimum(jnp.maximum(values, -reach), reach).astype(kind)


def setup_inputs(seed: int = 0) -> dict:
    seeds = jax.random.split(jax.random.key(seed), 10)
    right_side = draw_right_side(jax.random.fold_in(seeds[9], 71), 0)
    cell_level = place_ends(jax.random.randint(seeds[1], (CELLS,), 0, 4), jax.random.fold_in(seeds[1], 1), 0, 3).astype(jnp.int32)
    own_slot = place_ends(jax.random.randint(seeds[2], (ENTRIES,), 0, 6 * CELLS_DEV), jax.random.fold_in(seeds[2], 1), 0, (6 * CELLS_DEV) - 1).astype(jnp.int32)
    near_slot = draw_near_slot(jax.random.fold_in(seeds[9], 71), 0)
    face_kind = place_ends(jax.random.randint(seeds[4], (ENTRIES,), 0, 6), jax.random.fold_in(seeds[4], 1), 0, 5).astype(jnp.int32)
    orientation = place_ends(jax.random.randint(seeds[5], (ENTRIES,), 0, 8), jax.random.fold_in(seeds[5], 1), 0, 7).astype(jnp.int32)
    penalty = jnp.clip(jnp.exp(math.log(32.0) - 2.7725887 * jax.random.uniform(seeds[6], (ENTRIES,), jnp.float32) ** block_levels(seeds[6], (ENTRIES,), ((0, 32),), -0.2, 0.2)), 2.0, 32.0)
    send_slots = place_ends(jax.random.randint(seeds[7], (SENDS,), 0, 6 * CELLS_DEV), jax.random.fold_in(seeds[7], 1), 0, (6 * CELLS_DEV) - 1).astype(jnp.int32)
    subface_maps = centred(seeds[8], (4, NODES * NODES, NODES * NODES), (NODES * NODES) ** -0.5, 1.25, jnp.float32)
    return dict(right_side=right_side, cell_level=cell_level, own_slot=own_slot, near_slot=near_slot, face_kind=face_kind, orientation=orientation, penalty=penalty, send_slots=send_slots, subface_maps=subface_maps)


mass_shift = 1.0
curve_offsets = (1, -1, 2, -2)

def node_tables():
    points = np.array([-1.0, -np.sqrt(3.0 / 7.0), 0.0, np.sqrt(3.0 / 7.0), 1.0])
    weights = np.array([0.1, 49.0 / 90.0, 32.0 / 45.0, 49.0 / 90.0, 0.1])
    identity = np.eye(5)
    spacing = points[:, None] - points[None, :] + identity
    barycentric = 1.0 / np.prod(spacing, axis=1)
    offdiag = barycentric[None, :] / barycentric[:, None] / spacing
    diagonal = np.sum(1.0 / spacing, axis=1) - 1.0
    derivs = np.where(identity > 0.5, diagonal[:, None], offdiag)
    stiffness = derivs.T @ (weights[:, None] * derivs)
    return (jnp.asarray(stiffness, jnp.float32), jnp.asarray(weights, jnp.float32))

def volume_term(field, scale, tables):
    stiffness, weights = tables
    first = weights[:, None, None, None]
    second = weights[None, :, None, None]
    third = weights[None, None, :, None]
    along_first = jnp.einsum('ia,abcz->ibcz', stiffness, field, precision=lax.Precision.HIGHEST)
    along_second = jnp.einsum('jb,abcz->ajcz', stiffness, field, precision=lax.Precision.HIGHEST)
    along_third = jnp.einsum('kc,abcz->abkz', stiffness, field, precision=lax.Precision.HIGHEST)
    grads = along_first * second * third + along_second * first * third + along_third * first * second
    return scale * grads + mass_shift * scale * scale * scale * first * second * third * field

def face_traces(field):
    last = NODES - 1
    return jnp.stack([field[0], field[last], field[:, 0], field[:, last], field[:, :, 0], field[:, :, last]], axis=-2)

def lift_faces(faces):
    last = NODES - 1
    rest = faces.shape[2:-2] + faces.shape[-1:]
    volume = jnp.zeros((NODES, NODES, NODES) + rest, faces.dtype)
    volume = volume.at[0].add(faces[..., 0, :])
    volume = volume.at[last].add(faces[..., 1, :])
    volume = volume.at[:, 0].add(faces[..., 2, :])
    volume = volume.at[:, last].add(faces[..., 3, :])
    volume = volume.at[:, :, 0].add(faces[..., 4, :])
    volume = volume.at[:, :, last].add(faces[..., 5, :])
    return volume

def orient_forward(values, codes):
    values = jnp.where(codes & 1 == 1, values[::-1], values)
    values = jnp.where(codes & 2 == 2, values[:, ::-1], values)
    return jnp.where(codes & 4 == 4, jnp.swapaxes(values, 0, 1), values)

def orient_back(values, codes):
    values = jnp.where(codes & 4 == 4, jnp.swapaxes(values, 0, 1), values)
    values = jnp.where(codes & 2 == 2, values[:, ::-1], values)
    return jnp.where(codes & 1 == 1, values[::-1], values)

def map_traces(values, kinds, maps, transpose_maps):
    flat = values.reshape(NODES * NODES, -1)
    result = jnp.where(kinds == 1, flat, 0.0)
    for subface in range(4):
        matrix = maps[subface].T if transpose_maps else maps[subface]
        moved = jnp.dot(matrix, flat, precision=lax.Precision.HIGHEST)
        result = result + jnp.where(kinds == subface + 2, moved, 0.0)
    return result.reshape(values.shape)

def face_terms(own_values, near_values, kinds, orients, penalty, maps, weights):
    face_mass = weights[:, None, None] * weights[None, :, None]
    mapped = map_traces(orient_forward(near_values, orients), kinds, maps, False)
    jump = own_values - mapped
    own_term = penalty * face_mass * jump
    near_term = -orient_back(map_traces(own_term, kinds, maps, True), orients)
    return (own_term, near_term)

def shift_devices(blocks, offset):
    empty = jnp.zeros_like(blocks[:, :abs(offset)])
    if offset > 0:
        return jnp.concatenate([empty, blocks[:, :-offset]], axis=1)
    return jnp.concatenate([blocks[:, -offset:], empty], axis=1)

def apply_operator(field, scale, own_slot, near_slot, kinds, orients, penalty, send_slots, maps, tables):
    devices = N_SFC * N_GRP
    count = CELLS_DEV
    slots = 6 * count
    width = NODES * NODES
    span = slots + 4 * GHOST
    device_rows = jnp.arange(devices, dtype=jnp.int32)[:, None]
    traces = face_traces(field.reshape(NODES, NODES, NODES, devices, count)).reshape(width, devices * slots)
    send_index = (send_slots.reshape(devices, 4 * GHOST) + device_rows * slots).reshape(-1).astype(jnp.int32)
    sent = jnp.take(traces, send_index, axis=1).reshape(width, devices, 4, GHOST)
    arrived = [shift_devices(sent[:, :, position], offset) for position, offset in enumerate(curve_offsets)]
    ghosts = jnp.stack(arrived, axis=2).reshape(width, devices, 4 * GHOST)
    pool = jnp.concatenate([traces.reshape(width, devices, slots), ghosts], axis=2).reshape(width, devices * span)
    own_index = (own_slot.reshape(devices, -1) + device_rows * span).reshape(-1).astype(jnp.int32)
    near_index = (near_slot.reshape(devices, -1) + device_rows * span).reshape(-1).astype(jnp.int32)
    own_values = jnp.take(pool, own_index, axis=1).reshape(NODES, NODES, -1)
    near_values = jnp.take(pool, near_index, axis=1).reshape(NODES, NODES, -1)
    own_term, near_term = face_terms(own_values, near_values, kinds, orients, penalty, maps, tables[1])
    gathered = jnp.zeros_like(pool).at[:, own_index].add(own_term.reshape(width, -1))
    gathered = gathered.at[:, near_index].add(near_term.reshape(width, -1))
    gathered = gathered.reshape(width, devices, span)
    local = gathered[:, :, :slots].reshape(width, devices * slots)
    returned = gathered[:, :, slots:].reshape(width, devices, 4, GHOST)
    came_back = [shift_devices(returned[:, :, position], -offset) for position, offset in enumerate(curve_offsets)]
    back = jnp.stack(came_back, axis=2).reshape(width, devices * 4 * GHOST)
    local = local.at[:, send_index].add(back)
    faces = local.reshape(NODES, NODES, devices, 6, count)
    lifted = lift_faces(faces).reshape(NODES, NODES, NODES, devices * count)
    return volume_term(field, scale, tables) + lifted

def reference(right_side, cell_level, own_slot, near_slot, face_kind, orientation, penalty, send_slots, subface_maps):
    tables = node_tables()
    scale = jnp.exp2(-cell_level.astype(jnp.float32))
    devices = N_SFC * N_GRP
    device_rows = jnp.arange(devices, dtype=jnp.int32)[:, None]
    cell_index = (own_slot.reshape(devices, -1) % CELLS_DEV + device_rows * CELLS_DEV).reshape(-1).astype(jnp.int32)
    scaled_penalty = penalty * jnp.take(scale, cell_index)
    solution = jnp.zeros_like(right_side)
    residual = right_side
    direction = right_side
    norm_now = jnp.sum(residual * residual)
    for iteration in range(ITERS):
        image = apply_operator(direction, scale, own_slot, near_slot, face_kind, orientation, scaled_penalty, send_slots, subface_maps, tables)
        step_size = norm_now / jnp.sum(direction * image)
        solution = solution + step_size * direction
        residual = residual - step_size * image
        norm_next = jnp.sum(residual * residual)
        direction = residual + norm_next / norm_now * direction
        norm_now = norm_next
    return (solution, residual)
```

```python
import functools

import jax
import jax.numpy as jnp
import numpy as np
from jax import lax
from jax.experimental import pallas as pl
from jax.experimental.pallas import tpu as pltpu
from jax.sharding import PartitionSpec as P

NODES = 5
WIDTH = NODES * NODES
ROWS = 32
FACES = 6 * ROWS
CUBE = 208
ITERS = 3
MOMENTS = 2 * ITERS
MESSAGE = 56
UNIT = 2.0**-12
OFFSETS = (1, -1, 2, -2)
MASS = 1.0
MESH = pl.DeviceIdType.MESH
F32 = jnp.float32
BF16 = jnp.bfloat16


def node_tables():
    points = np.array([-1.0, -np.sqrt(3.0 / 7.0), 0.0, np.sqrt(3.0 / 7.0), 1.0])
    weights = np.array([0.1, 49.0 / 90.0, 32.0 / 45.0, 49.0 / 90.0, 0.1])
    identity = np.eye(5)
    spacing = points[:, None] - points[None, :] + identity
    barycentric = 1.0 / np.prod(spacing, axis=1)
    offdiag = barycentric[None, :] / barycentric[:, None] / spacing
    diagonal = np.sum(1.0 / spacing, axis=1) - 1.0
    derivs = np.where(identity > 0.5, diagonal[:, None], offdiag)
    return derivs.T @ (weights[:, None] * derivs), weights


def constants():
    stiff, w = node_tables()
    mass = np.diag(w)
    kron = lambda a, b, c: np.kron(np.kron(a, b), c)
    spots = (np.arange(WIDTH)[:, None] * 8 + np.arange(NODES)).reshape(-1)
    nodes = spots.reshape(5, 5, 5)
    layers = [nodes[0], nodes[4], nodes[:, 0], nodes[:, 4], nodes[:, :, 0], nodes[:, :, 4]]
    select = np.zeros((FACES, CUBE))
    for face, layer in enumerate(layers):
        select[face * ROWS + np.arange(WIDTH), layer.reshape(-1)] = 1.0
    both = np.concatenate([select, np.eye(CUBE)])
    volume = np.zeros((CUBE, CUBE))
    volume[np.ix_(spots, spots)] = kron(stiff, mass, mass) + kron(mass, stiff, mass) + kron(mass, mass, stiff)
    volume = both @ volume * UNIT
    high = volume.astype(jnp.bfloat16)
    low = (volume - high.astype(np.float64)).astype(jnp.bfloat16)
    volume = np.concatenate([high, high, low], axis=1)
    lift = both @ select.T
    lift = np.concatenate([lift, lift], axis=1)
    turn = np.zeros((8, ROWS, ROWS))
    for code in range(8):
        order = np.arange(WIDTH).reshape(5, 5)
        order = order[::-1] if code & 1 else order
        order = order[:, ::-1] if code & 2 else order
        order = order.T if code & 4 else order
        turn[code, np.arange(WIDTH), order.reshape(-1)] = 1.0
    back = np.swapaxes(turn, 1, 2)
    turns = np.concatenate([np.concatenate([m, m], axis=2).reshape(8 * ROWS, 2 * ROWS) for m in (turn, back)])
    face_mass = np.zeros((ROWS, 128))
    face_mass[:WIDTH] = UNIT * np.outer(w, w).reshape(-1, 1)
    cube_mass = np.zeros((CUBE, 128))
    cube_mass[spots] = UNIT * MASS * np.einsum("a,b,c->abc", w, w, w).reshape(-1, 1)
    bf = lambda a: jnp.asarray(np.asarray(a, np.float32), BF16)
    return (
        bf(select),
        bf(turns),
        jnp.asarray(np.concatenate([face_mass, both @ cube_mass]), F32),
        bf(volume),
        bf(lift),
    )


def high_low(x):
    high = x.astype(BF16).astype(F32)
    return high, x - high


def split(x):
    high = x.astype(BF16)
    return high, (x - high.astype(F32)).astype(BF16)


def dot(a, b):
    return jnp.dot(a, b, preferred_element_type=F32)


def dot_nt(a, b):
    return lax.dot_general(a, b, (((1,), (1,)), ((), ())), preferred_element_type=F32)


def ring_levels(total):
    levels, stride = [], 1
    while stride < total:
        rest = total // stride
        size = max(g for g in range(1, 33) if rest % g == 0)
        size = rest if size == 1 else size
        levels.append((stride, size))
        stride *= size
    return levels


def conjugate(m):
    def inner(a, b, shift):
        total = None
        for power in range(len(a) + len(b) - 1):
            weight = sum(a[i] * b[power - i] for i in range(len(a)) if 0 <= power - i < len(b))
            term = weight * m[power + shift]
            total = term if total is None else total + term
        return total

    one = jnp.ones_like(m[0])
    x, r, p = [], [one], [one]
    norm = m[0]
    for it in range(ITERS):
        alpha = norm / inner(p, p, 1)
        x = [(x[i] if i < len(x) else 0.0) + alpha * p[i] for i in range(len(p))]
        r = [one] + [-value for value in x]
        if it + 1 < ITERS:
            new = inner(r, r, 0)
            beta = new / norm
            p = [r[i] + (beta * p[i] if i < len(p) else 0.0) for i in range(len(r))]
            norm = new
    return x


def kernel(
    dims,
    rhs_hbm, level_hbm, own_hbm, near_hbm, kind_hbm, orient_hbm, pen_hbm, send_hbm, maps_hbm,
    sel_hbm, turn_hbm, mass_hbm, vol_hbm, lift_hbm,
    x_out, r_out,
    rhs_ref, level_ref, own_ref, near_ref, kind_ref, orient_ref, pen_ref, send_ref, maps_ref,
    sel_ref, turn_ref, mass_ref, vol_ref, lift_ref,
    cells, cells_t, marks, mapz, diag, xsrc, xbuf, asrc, *rest,
):
    n_sfc, n_grp, count, ghost, pad = dims
    total = n_sfc * n_grp
    levels = ring_levels(total)
    slots_refs = rest[: len(levels)]
    insem, xsend, xrecv, asend, arecv = rest[len(levels):]
    me = lax.axis_index("sfc") * n_grp + lax.axis_index("grp")
    slots = 6 * count
    entries = 4 * ghost
    cols = 4 * pad

    loads = {}
    for i, (name, src, dst) in enumerate([
        ("near", near_hbm, near_ref), ("own", own_hbm, own_ref), ("send", send_hbm, send_ref),
        ("level", level_hbm, level_ref), ("rhs", rhs_hbm, rhs_ref), ("sel", sel_hbm, sel_ref),
        ("kind", kind_hbm, kind_ref), ("orient", orient_hbm, orient_ref), ("pen", pen_hbm, pen_ref),
        ("turn", turn_hbm, turn_ref), ("mass", mass_hbm, mass_ref), ("maps", maps_hbm, maps_ref),
        ("vol", vol_hbm, vol_ref), ("lift", lift_hbm, lift_ref),
    ]):
        loads[name] = pltpu.make_async_copy(src, dst, insem.at[i])
        loads[name].start()

    def place(device):
        return (device // n_grp, lax.rem(device, n_grp))

    def near_device(k):
        return place(lax.rem(me + OFFSETS[k] + total, total))

    def peer(level, step):
        stride, size = levels[level]
        digit = lax.rem(me // stride, size)
        return place(me + (lax.rem(digit + step, size) - digit) * stride)

    exists = [(me + offset >= 0) & (me + offset < total) for offset in OFFSETS]

    def guarded(k, action):
        @pl.when(exists[k])
        def _():
            action()

    barrier = pltpu.get_barrier_semaphore()
    greeted = 0
    for level, (_, size) in enumerate(levels):
        def greet(step, carry, level=level):
            pl.semaphore_signal(barrier, inc=1, device_id=peer(level, step), device_id_type=MESH)
            return carry
        lax.fori_loop(1, size, greet, 0)
        greeted += size - 1
    if len(levels) > 1:
        for k in range(4):
            pl.semaphore_signal(barrier, inc=1, device_id=near_device(k), device_id_type=MESH)
        greeted += 4

    for k in range(4):
        @pl.when(jnp.logical_not(exists[k]))
        def _(k=k):
            for it in range(ITERS):
                xbuf[it, k] = jnp.zeros(xbuf.shape[2:], F32)

    for name in ("near", "own", "send", "level", "rhs", "sel", "kind", "orient", "pen"):
        loads[name].wait()
    line = lambda ref: ref[...].reshape(1, -1)

    inner = lax.broadcasted_iota(jnp.int32, (WIDTH, 8, count), 1) < NODES
    padded = jnp.concatenate([rhs_ref[...], jnp.zeros((WIDTH, 8 - NODES, count), F32)], axis=1)
    field = jnp.concatenate(
        [jnp.where(inner, padded, 0.0).reshape(WIDTH * 8, count), jnp.zeros((CUBE - WIDTH * 8, count), F32)], axis=0
    )
    field_high, field_low = split(field)
    picked = dot(sel_ref[...], jnp.concatenate([field_high, field_low], axis=1))
    scale = jnp.exp2(-line(level_ref).astype(F32))
    face_row = lax.rem(lax.broadcasted_iota(jnp.int32, (FACES, count), 0), ROWS)
    trace_high = jnp.where(face_row == WIDTH, scale, picked[:, :count])
    trace_low = picked[:, count:]

    own = line(own_ref)
    pen = line(pen_ref)
    pen_a, pen_b = high_low(pen)
    pen_b, pen_c = high_low(pen_b)
    send = line(send_ref)
    zero_row = jnp.zeros_like(pen)
    rows = [(own >> 8).astype(F32), (own & 255).astype(F32), line(kind_ref).astype(F32), line(orient_ref).astype(F32)]
    params = jnp.concatenate(rows + [pen_a, pen_b, pen_c, zero_row], axis=0).astype(BF16)
    sent_rows = jnp.concatenate([(send >> 8).astype(F32), (send & 255).astype(F32)] + [zero_row] * 6, axis=0).astype(BF16)
    near = jnp.broadcast_to(line(near_ref), (pad, entries))
    spot = lax.broadcasted_iota(jnp.int32, (pad, entries), 0)
    lane = lax.broadcasted_iota(jnp.int32, (pad, entries), 1)
    inside = spot < ghost
    order, spread = [], []
    for k in range(4):
        order.append(jnp.where(inside & (near == spot + (slots + k * ghost)), 1.0, 0.0).astype(BF16))
        spread.append(jnp.where(inside & (lane == spot + k * ghost), 1.0, 0.0).astype(BF16))
    ordered = dot_nt(params, jnp.concatenate(order, axis=0))
    spread = dot_nt(sent_rows, jnp.concatenate(spread, axis=0))
    slot = jnp.concatenate(
        [spread[0:1] * 256.0 + spread[1:2], ordered[0:1] * 256.0 + ordered[1:2]], axis=1
    ).astype(jnp.int32)
    face = jnp.zeros_like(slot)
    for f in range(1, 6):
        face = face + jnp.where(slot >= f * count, 1, 0)
    cell = slot - face * count
    cell_row = lax.broadcasted_iota(jnp.int32, (count, 2 * cols), 0)
    chosen = jnp.where(cell_row == cell, 1.0, 0.0)
    cells[:count] = chosen.astype(BF16)
    cells[count:] = chosen.astype(BF16)

    def gather(high, low):
        found = dot(jnp.concatenate([high, low], axis=1).astype(BF16), cells[...])
        raw = found[:ROWS]
        for f in range(1, 6):
            raw = jnp.where(face == f, found[f * ROWS : (f + 1) * ROWS], raw)
        return raw

    raw = gather(trace_high, trace_low)
    strength = (ordered[4:5] + ordered[5:6] + ordered[6:7]) * raw[WIDTH : WIDTH + 1, cols:]
    sub = lax.broadcasted_iota(jnp.int32, (8, cols), 0)
    tail = jnp.where(sub == 0, ordered[2:3], jnp.where(sub == 1, ordered[3:4], jnp.where(sub == 2, strength, 0.0)))

    pl.semaphore_wait(barrier, greeted)

    xcopies = []

    def send_out(turn_number, raw):
        count_rows = MESSAGE if turn_number == 0 else 2 * WIDTH
        copies = []
        for k in range(4):
            other = cols + (k ^ 1) * pad
            xsrc[turn_number, k, :WIDTH] = raw[:WIDTH, k * pad : (k + 1) * pad]
            xsrc[turn_number, k, WIDTH : 2 * WIDTH] = raw[:WIDTH, other : other + pad]
            if turn_number == 0:
                xsrc[turn_number, k, 2 * WIDTH :] = tail[: MESSAGE - 2 * WIDTH, other - cols : other - cols + pad]
            copies.append(pltpu.make_async_remote_copy(
                src_ref=xsrc.at[turn_number, k, pl.ds(0, count_rows)],
                dst_ref=xbuf.at[turn_number, k ^ 1, pl.ds(0, count_rows)],
                send_sem=xsend.at[turn_number, k], recv_sem=xrecv.at[turn_number, k ^ 1],
                device_id=near_device(k), device_id_type=MESH,
            ))
        for k in (2, 3, 0, 1):
            guarded(k, copies[k].start)
        xcopies.append(copies)

    send_out(0, raw)

    for name in ("turn", "mass", "maps", "vol", "lift"):
        loads[name].wait()
    for f in range(6):
        marks[f] = jnp.broadcast_to(jnp.where(face == f, 1.0, 0.0), (16, 2 * cols)).astype(BF16)
    cells_t[...] = chosen.T.astype(BF16)
    mapz[...] = jnp.zeros_like(mapz)
    for s in range(4):
        mapz[s * ROWS : s * ROWS + WIDTH, 0:WIDTH] = maps_ref[:, s, :]
    maps = mapz[...]
    transposed = maps.T
    backs = jnp.concatenate([transposed[:ROWS, s * ROWS : (s + 1) * ROWS] for s in range(4)], axis=0)

    def three(matrix):
        high, low = split(matrix)
        return jnp.concatenate([high, high, low], axis=1)

    forward = three(maps[:, :ROWS])
    backward = three(backs)
    face_mass = jnp.concatenate([mass_ref[:ROWS]] * (cols // 128), axis=1)
    diag[:, cols:] = face_mass * strength
    mass_scale = mass_ref[ROWS:] * (scale * scale * scale)

    def turned(values, codes, table):
        forms = dot(table, jnp.concatenate(split(values), axis=0))
        result = forms[:ROWS]
        for code in range(1, 8):
            result = jnp.where(codes == code, forms[code * ROWS : (code + 1) * ROWS], result)
        return result

    def mapped(values, kinds, table):
        high, low = split(values)
        forms = dot(table, jnp.concatenate([high, low, high], axis=0))
        result = jnp.where(kinds == 1, values, 0.0)
        for s in range(4):
            result = jnp.where(kinds == s + 2, forms[s * ROWS : (s + 1) * ROWS], result)
        return result

    turn_table = turn_ref[: 8 * ROWS]
    back_table = turn_ref[8 * ROWS :]
    own_kinds = ordered[2:3].astype(jnp.int32)
    own_codes = ordered[3:4].astype(jnp.int32)

    def image_of(state, high, low, first):
        flat = jnp.concatenate([high, low, high], axis=0)
        return dot(vol_ref[first:], flat) * scale + mass_scale[first:] * state

    def sum_all(a):
        return jnp.sum(jnp.sum(a, axis=0, keepdims=True), axis=1, keepdims=True)

    def level_copy(level, step):
        return pltpu.make_async_remote_copy(
            src_ref=asrc.at[level], dst_ref=slots_refs[level].at[step - 1],
            send_sem=asend.at[level], recv_sem=arecv.at[level],
            device_id=peer(level, step), device_id_type=MESH,
        )

    def level_start(level):
        def start(step, carry):
            level_copy(level, step).start()
            return carry
        lax.fori_loop(1, levels[level][1], start, 0)

    basis = [field]
    moments = [sum_all(field * field)]
    state = jnp.concatenate([trace_high + trace_low, field], axis=0)
    mine = None
    for it in range(ITERS):
        last = it + 1 == ITERS
        first = FACES if last else 0
        image = image_of(state[first:], field_high, field_low, first)
        near_raw, own_raw = raw[:, :cols], raw[:, cols:]
        if it:
            mine = mapped(turned(near_raw, near_codes, turn_table), near_kinds, forward)
        for k in range(4):
            guarded(k ^ 1, xcopies[it][k].wait_recv)
        filler = jnp.zeros((ROWS - WIDTH, cols), F32)
        near_got = jnp.concatenate([xbuf[it, k ^ 1, :ROWS] for k in range(4)], axis=1)
        own_got = jnp.concatenate([xbuf[it, k, WIDTH : 2 * WIDTH] for k in range(4)], axis=1)
        own_got = jnp.concatenate([own_got, filler], axis=0)
        if it == 0:
            info = [
                jnp.concatenate([xbuf[it, k, 2 * WIDTH + i : 2 * WIDTH + i + 1] for k in range(4)], axis=1)
                for i in range(3)
            ]
            near_kinds = info[0].astype(jnp.int32)
            near_codes = info[1].astype(jnp.int32)
            diag[:, :cols] = face_mass * info[2]
            mine = mapped(turned(near_raw, near_codes, turn_table), near_kinds, forward)
        theirs = mapped(turned(near_got, own_codes, turn_table), own_kinds, forward)
        jump = own_raw - theirs
        own_flux = diag[:, cols:] * jump
        if last:
            moments.append(sum_all(field * image) + sum_all(own_flux * jump))
            lane_row = lax.broadcasted_iota(jnp.int32, (1, 128), 1)
            row = jnp.zeros((1, 128), F32)
            for i, part in enumerate(moments):
                row = jnp.where(lane_row == i, part, row)
            asrc[0] = row
            level_start(0)
        near_flux = diag[:, :cols] * (mine - own_got)
        near_flux = turned(mapped(near_flux, near_kinds, backward), near_codes, back_table)
        flux = jnp.concatenate([near_flux, own_flux], axis=1)
        parts = []
        for part in split(flux):
            for f in range(6):
                for half in range(ROWS // 16):
                    parts.append(part[half * 16 : (half + 1) * 16] * marks[f])
        faces = dot(jnp.concatenate(parts, axis=0), cells_t[...])
        faces = faces[:FACES] + faces[FACES:]
        new = image + dot(lift_ref[first:], jnp.concatenate(split(faces), axis=0))
        if last:
            basis.append(new)
            break
        state = new
        trace = state[:FACES]
        trace_high, trace_low = high_low(trace)
        raw = gather(trace_high, trace_low)
        send_out(it + 1, raw)
        field = state[FACES:]
        field_high, field_low = split(field)
        moments.append(sum_all(basis[-1] * field))
        moments.append(sum_all(field * field))
        basis.append(field)

    for level in range(len(levels)):
        landed = slots_refs[level]
        pltpu.make_async_copy(landed, landed, arecv.at[level]).wait()
        value = asrc[level] + jnp.sum(landed[...], axis=0)
        if level + 1 < len(levels):
            asrc[level + 1] = value
            level_start(level + 1)
    value = jnp.broadcast_to(value, (8, 128))
    coefs = conjugate([jnp.broadcast_to(value[:, i : i + 1], (8, count)) for i in range(MOMENTS)])
    cubes = [v[: WIDTH * 8].reshape(WIDTH, 8, count) for v in basis]
    x = coefs[0] * cubes[0]
    r = cubes[0] - coefs[0] * cubes[1]
    for i in range(1, ITERS):
        x = x + coefs[i] * cubes[i]
        r = r - coefs[i] * cubes[i + 1]
    x_out[...] = (UNIT * x)[:, :NODES]
    r_out[...] = r[:, :NODES]

    for copies in xcopies:
        for k in range(4):
            guarded(k, copies[k].wait_send)
    for level in range(len(levels)):
        landed = slots_refs[level]
        pltpu.make_async_copy(landed, landed, asend.at[level]).wait()


def body(n_sfc, n_grp, right_side, cell_level, own_slot, near_slot, face_kind, orientation, penalty, send_slots, maps):
    count = right_side.shape[-1]
    ghost = send_slots.shape[0] // 4
    pad = -(-ghost // 128) * 128
    levels = ring_levels(n_sfc * n_grp)
    dma = pltpu.SemaphoreType.DMA
    shape = jax.ShapeDtypeStruct((WIDTH, NODES, count), F32)
    operands = (
        right_side.reshape(WIDTH, NODES, count),
        cell_level, own_slot, near_slot, face_kind, orientation, penalty, send_slots,
        jnp.swapaxes(maps, 0, 1), *constants(),
    )
    vmem = pl.BlockSpec(memory_space=pltpu.VMEM)
    x, r = pl.pallas_call(
        functools.partial(kernel, (n_sfc, n_grp, count, ghost, pad)),
        out_shape=(shape, shape),
        in_specs=[pl.BlockSpec(memory_space=pltpu.HBM)] * len(operands),
        out_specs=(vmem, vmem),
        scratch_shapes=[pltpu.VMEM(operand.shape, operand.dtype) for operand in operands]
        + [
            pltpu.VMEM((2 * count, 8 * pad), BF16),
            pltpu.VMEM((8 * pad, count), BF16),
            pltpu.VMEM((6, 16, 8 * pad), BF16),
            pltpu.VMEM((4 * ROWS, 128), F32),
            pltpu.VMEM((ROWS, 8 * pad), F32),
            pltpu.VMEM((ITERS, 4, MESSAGE, pad), F32),
            pltpu.VMEM((ITERS, 4, MESSAGE, pad), F32),
            pltpu.VMEM((len(levels), 1, 128), F32),
        ]
        + [pltpu.VMEM((size - 1, 1, 128), F32) for _, size in levels]
        + [
            dma((len(operands),)),
            dma((ITERS, 4)),
            dma((ITERS, 4)),
            dma((len(levels),)),
            dma((len(levels),)),
        ],
        compiler_params=pltpu.CompilerParams(
            collective_id=0, has_side_effects=True
        ),
    )(*operands)
    return x.reshape(right_side.shape), r.reshape(right_side.shape)


def solution(mesh):
    split_spec = P(("sfc", "grp"))
    field_spec = P(None, None, None, ("sfc", "grp"))
    return jax.shard_map(
        functools.partial(body, mesh.shape["sfc"], mesh.shape["grp"]),
        mesh=mesh,
        in_specs=(field_spec,) + (split_spec,) * 7 + (P(),),
        out_specs=(field_spec, field_spec),
        check_vma=False,
    )
```

```python
import functools

import jax
import jax.numpy as jnp
import numpy as np
from jax import lax
from jax.experimental import pallas as pl
from jax.experimental.pallas import tpu as pltpu
from jax.sharding import PartitionSpec as P

NODES = 5
WIDTH = NODES * NODES
ROWS = 32
FACES = 6 * ROWS
CUBE = 208
ITERS = 3
MOMENTS = 2 * ITERS
MESSAGE = 56
UNIT = 2.0**-12
OFFSETS = (1, -1, 2, -2)
MASS = 1.0
LOGICAL = pl.DeviceIdType.LOGICAL
F32 = jnp.float32
BF16 = jnp.bfloat16


def node_tables():
    points = np.array([-1.0, -np.sqrt(3.0 / 7.0), 0.0, np.sqrt(3.0 / 7.0), 1.0])
    weights = np.array([0.1, 49.0 / 90.0, 32.0 / 45.0, 49.0 / 90.0, 0.1])
    identity = np.eye(5)
    spacing = points[:, None] - points[None, :] + identity
    barycentric = 1.0 / np.prod(spacing, axis=1)
    offdiag = barycentric[None, :] / barycentric[:, None] / spacing
    diagonal = np.sum(1.0 / spacing, axis=1) - 1.0
    derivs = np.where(identity > 0.5, diagonal[:, None], offdiag)
    return derivs.T @ (weights[:, None] * derivs), weights


def constants():
    stiff, w = node_tables()
    mass = np.diag(w)
    kron = lambda a, b, c: np.kron(np.kron(a, b), c)
    spots = (np.arange(WIDTH)[:, None] * 8 + np.arange(NODES)).reshape(-1)
    nodes = spots.reshape(5, 5, 5)
    layers = [nodes[0], nodes[4], nodes[:, 0], nodes[:, 4], nodes[:, :, 0], nodes[:, :, 4]]
    select = np.zeros((FACES, CUBE))
    for face, layer in enumerate(layers):
        select[face * ROWS + np.arange(WIDTH), layer.reshape(-1)] = 1.0
    both = np.concatenate([select, np.eye(CUBE)])
    volume = np.zeros((CUBE, CUBE))
    volume[np.ix_(spots, spots)] = kron(stiff, mass, mass) + kron(mass, stiff, mass) + kron(mass, mass, stiff)
    volume = both @ volume * UNIT
    high = volume.astype(jnp.bfloat16)
    low = (volume - high.astype(np.float64)).astype(jnp.bfloat16)
    volume = np.concatenate([high, low])
    lift = both @ select.T
    turn = np.zeros((8, ROWS, ROWS))
    for code in range(8):
        order = np.arange(WIDTH).reshape(5, 5)
        order = order[::-1] if code & 1 else order
        order = order[:, ::-1] if code & 2 else order
        order = order.T if code & 4 else order
        turn[code, np.arange(WIDTH), order.reshape(-1)] = 1.0
    back = np.swapaxes(turn, 1, 2)
    turns = np.concatenate([np.concatenate([m, m], axis=2).reshape(8 * ROWS, 2 * ROWS) for m in (turn, back)])
    face_mass = np.zeros((ROWS, 128))
    face_mass[:WIDTH] = UNIT * np.outer(w, w).reshape(-1, 1)
    cube_mass = np.zeros((CUBE, 128))
    cube_mass[spots] = UNIT * MASS * np.einsum("a,b,c->abc", w, w, w).reshape(-1, 1)
    bf = lambda a: jnp.asarray(np.asarray(a, np.float32), BF16)
    return (
        bf(select),
        bf(turns),
        jnp.asarray(np.concatenate([face_mass, both @ cube_mass]), F32),
        bf(volume),
        bf(lift),
    )


def high_low(x):
    high = x.astype(BF16).astype(F32)
    return high, x - high


def split(x):
    high = x.astype(BF16)
    return high, (x - high.astype(F32)).astype(BF16)


def dot(a, b):
    return jnp.dot(a, b, preferred_element_type=F32)


def dot_nt(a, b):
    return lax.dot_general(a, b, (((1,), (1,)), ((), ())), preferred_element_type=F32)


def ring_levels(total):
    levels, stride = [], 1
    while stride < total:
        rest = total // stride
        size = max(g for g in range(1, 33) if rest % g == 0)
        size = rest if size == 1 else size
        levels.append((stride, size))
        stride *= size
    return levels


def conjugate(m):
    def inner(a, b, shift):
        total = None
        for power in range(len(a) + len(b) - 1):
            weight = sum(a[i] * b[power - i] for i in range(len(a)) if 0 <= power - i < len(b))
            term = weight * m[power + shift]
            total = term if total is None else total + term
        return total

    one = jnp.ones_like(m[0])
    x, r, p = [], [one], [one]
    norm = m[0]
    for it in range(ITERS):
        alpha = norm / inner(p, p, 1)
        x = [(x[i] if i < len(x) else 0.0) + alpha * p[i] for i in range(len(p))]
        r = [one] + [-value for value in x]
        if it + 1 < ITERS:
            new = inner(r, r, 0)
            beta = new / norm
            p = [r[i] + (beta * p[i] if i < len(p) else 0.0) for i in range(len(r))]
            norm = new
    return x


def kernel(
    dims,
    rhs_hbm, level_hbm, own_hbm, near_hbm, kind_hbm, orient_hbm, pen_hbm, send_hbm, maps_hbm,
    sel_hbm, turn_hbm, mass_hbm, vol_hbm, lift_hbm,
    x_out, r_out,
    rhs_ref, level_ref, own_ref, near_ref, kind_ref, orient_ref, pen_ref, send_ref, maps_ref,
    sel_ref, turn_ref, mass_ref, vol_ref, lift_ref,
    cells, cells_t, marks, mapz, diag, xsrc, xbuf, asrc, *rest,
):
    n_sfc, n_grp, count, ghost, pad = dims
    total = n_sfc * n_grp
    levels = ring_levels(total)
    slots_refs = rest[: len(levels)]
    insem, xsend, xrecv, asend, arecv = rest[len(levels):]
    me = lax.axis_index("sfc") * n_grp + lax.axis_index("grp")
    slots = 6 * count
    entries = 4 * ghost
    cols = 4 * pad

    loads = {}
    for i, (name, src, dst) in enumerate([
        ("near", near_hbm, near_ref), ("own", own_hbm, own_ref), ("send", send_hbm, send_ref),
        ("level", level_hbm, level_ref), ("rhs", rhs_hbm, rhs_ref), ("sel", sel_hbm, sel_ref),
        ("kind", kind_hbm, kind_ref), ("orient", orient_hbm, orient_ref), ("pen", pen_hbm, pen_ref),
        ("turn", turn_hbm, turn_ref), ("mass", mass_hbm, mass_ref), ("maps", maps_hbm, maps_ref),
        ("vol", vol_hbm, vol_ref), ("lift", lift_hbm, lift_ref),
    ]):
        loads[name] = pltpu.make_async_copy(src, dst, insem.at[i])
        loads[name].start()

    exists = [(me + offset >= 0) & (me + offset < total) for offset in OFFSETS]

    def near_device(k):
        return me + jnp.where(exists[k], OFFSETS[k], 0)

    digits = [lax.rem(me // stride, size) for stride, size in levels]

    def peer(level, step):
        stride, size = levels[level]
        return me + jnp.where(digits[level] + step >= size, step - size, step) * stride

    def guarded(k, action):
        @pl.when(exists[k])
        def _():
            action()

    barrier = pltpu.get_barrier_semaphore()
    greeted = 0
    for level, (_, size) in enumerate(levels):
        for step in range(1, size):
            pl.semaphore_signal(barrier, inc=1, device_id=peer(level, step), device_id_type=LOGICAL)
        greeted += size - 1
    if len(levels) > 1:
        for k in range(4):
            pl.semaphore_signal(barrier, inc=1, device_id=near_device(k), device_id_type=LOGICAL)
        greeted += 4

    for k in range(4):
        @pl.when(jnp.logical_not(exists[k]))
        def _(k=k):
            for it in range(ITERS):
                xbuf[it, k] = jnp.zeros(xbuf.shape[2:], F32)

    for name in ("near", "own", "send", "level", "rhs", "sel", "kind", "orient", "pen"):
        loads[name].wait()
    line = lambda ref: ref[...].reshape(1, -1)

    inner = lax.broadcasted_iota(jnp.int32, (WIDTH, 8, count), 1) < NODES
    padded = jnp.concatenate([rhs_ref[...], jnp.zeros((WIDTH, 8 - NODES, count), F32)], axis=1)
    field = jnp.concatenate(
        [jnp.where(inner, padded, 0.0).reshape(WIDTH * 8, count), jnp.zeros((CUBE - WIDTH * 8, count), F32)], axis=0
    )
    field_high, field_low = split(field)
    picked = dot(sel_ref[...], jnp.concatenate([field_high, field_low], axis=1))
    scale = jnp.exp2(-line(level_ref).astype(F32))
    face_row = lax.rem(lax.broadcasted_iota(jnp.int32, (FACES, count), 0), ROWS)
    trace_high = jnp.where(face_row == WIDTH, scale, picked[:, :count])
    trace_low = picked[:, count:]

    own = line(own_ref)
    pen = line(pen_ref)
    pen_a, pen_b = high_low(pen)
    pen_b, pen_c = high_low(pen_b)
    send = line(send_ref)
    zero_row = jnp.zeros_like(pen)
    rows = [(own >> 8).astype(F32), (own & 255).astype(F32), line(kind_ref).astype(F32), line(orient_ref).astype(F32)]
    params = jnp.concatenate(rows + [pen_a, pen_b, pen_c, zero_row], axis=0).astype(BF16)
    sent_rows = jnp.concatenate([(send >> 8).astype(F32), (send & 255).astype(F32)] + [zero_row] * 6, axis=0).astype(BF16)
    near = jnp.broadcast_to(line(near_ref), (pad, entries))
    spot = lax.broadcasted_iota(jnp.int32, (pad, entries), 0)
    lane = lax.broadcasted_iota(jnp.int32, (pad, entries), 1)
    inside = spot < ghost
    order, spread = [], []
    for k in range(4):
        order.append(jnp.where(inside & (near == spot + (slots + k * ghost)), 1.0, 0.0).astype(BF16))
        spread.append(jnp.where(inside & (lane == spot + k * ghost), 1.0, 0.0).astype(BF16))
    ordered = dot_nt(params, jnp.concatenate(order, axis=0))
    spread = dot_nt(sent_rows, jnp.concatenate(spread, axis=0))
    slot = jnp.concatenate(
        [spread[0:1] * 256.0 + spread[1:2], ordered[0:1] * 256.0 + ordered[1:2]], axis=1
    ).astype(jnp.int32)
    face = jnp.zeros_like(slot)
    for f in range(1, 6):
        face = face + jnp.where(slot >= f * count, 1, 0)
    cell = slot - face * count
    cell_row = lax.broadcasted_iota(jnp.int32, (count, 2 * cols), 0)
    chosen = jnp.where(cell_row == cell, 1.0, 0.0)
    cells[:count] = chosen.astype(BF16)
    cells[count:] = chosen.astype(BF16)

    def gather(high, low):
        found = dot(jnp.concatenate([high, low], axis=1).astype(BF16), cells[...])
        raw = found[:ROWS]
        for f in range(1, 6):
            raw = jnp.where(face == f, found[f * ROWS : (f + 1) * ROWS], raw)
        return raw

    raw = gather(trace_high, trace_low)
    strength = (ordered[4:5] + ordered[5:6] + ordered[6:7]) * raw[WIDTH : WIDTH + 1, cols:]
    sub = lax.broadcasted_iota(jnp.int32, (8, cols), 0)
    tail = jnp.where(sub == 0, ordered[2:3], jnp.where(sub == 1, ordered[3:4], jnp.where(sub == 2, strength, 0.0)))

    pl.semaphore_wait(barrier, greeted)

    xcopies = []

    def send_out(turn_number, raw):
        count_rows = MESSAGE if turn_number == 0 else 2 * WIDTH
        copies = []
        for k in range(4):
            other = cols + (k ^ 1) * pad
            xsrc[turn_number, k, :WIDTH] = raw[:WIDTH, k * pad : (k + 1) * pad]
            xsrc[turn_number, k, WIDTH : 2 * WIDTH] = raw[:WIDTH, other : other + pad]
            if turn_number == 0:
                xsrc[turn_number, k, 2 * WIDTH :] = tail[: MESSAGE - 2 * WIDTH, other - cols : other - cols + pad]
            copies.append(pltpu.make_async_remote_copy(
                src_ref=xsrc.at[turn_number, k, pl.ds(0, count_rows)],
                dst_ref=xbuf.at[turn_number, k ^ 1, pl.ds(0, count_rows)],
                send_sem=xsend.at[turn_number, k], recv_sem=xrecv.at[turn_number, k ^ 1],
                device_id=near_device(k), device_id_type=LOGICAL,
            ))
        for k in (2, 3, 0, 1):
            guarded(k, copies[k].start)
        xcopies.append(copies)

    send_out(0, raw)

    for name in ("turn", "mass", "maps", "vol", "lift"):
        loads[name].wait()
    for f in range(6):
        marks[f] = jnp.broadcast_to(jnp.where(face == f, 1.0, 0.0), (16, 2 * cols)).astype(BF16)
    cells_t[...] = chosen.T.astype(BF16)
    mapz[...] = jnp.zeros_like(mapz)
    for s in range(4):
        mapz[s * ROWS : s * ROWS + WIDTH, 0:WIDTH] = maps_ref[:, s, :]
    maps = mapz[...]
    transposed = maps.T
    backs = jnp.concatenate([transposed[:ROWS, s * ROWS : (s + 1) * ROWS] for s in range(4)], axis=0)

    def three(matrix):
        high, low = split(matrix)
        return jnp.concatenate([high, high, low], axis=1)

    forward = three(maps[:, :ROWS])
    backward = three(backs)
    face_mass = jnp.concatenate([mass_ref[:ROWS]] * (cols // 128), axis=1)
    diag[:, cols:] = face_mass * strength
    mass_scale = mass_ref[ROWS:] * (scale * scale * scale)

    def turned(values, codes, table):
        forms = dot(table, jnp.concatenate(split(values), axis=0))
        result = forms[:ROWS]
        for code in range(1, 8):
            result = jnp.where(codes == code, forms[code * ROWS : (code + 1) * ROWS], result)
        return result

    def mapped(values, kinds, table):
        high, low = split(values)
        forms = dot(table, jnp.concatenate([high, low, high], axis=0))
        result = jnp.where(kinds == 1, values, 0.0)
        for s in range(4):
            result = jnp.where(kinds == s + 2, forms[s * ROWS : (s + 1) * ROWS], result)
        return result

    turn_table = turn_ref[: 8 * ROWS]
    back_table = turn_ref[8 * ROWS :]
    own_kinds = ordered[2:3].astype(jnp.int32)
    own_codes = ordered[3:4].astype(jnp.int32)

    def image_of(state, high, low, first):
        both = dot(vol_ref[first : FACES + CUBE], jnp.concatenate([high, low], axis=1))
        both = both[:, :count] + both[:, count:] + dot(vol_ref[FACES + CUBE + first :], high)
        return both * scale + mass_scale[first:] * state

    def sum_all(a):
        return jnp.sum(jnp.sum(a, axis=0, keepdims=True), axis=1, keepdims=True)

    def level_copy(level, step):
        return pltpu.make_async_remote_copy(
            src_ref=asrc.at[level], dst_ref=slots_refs[level].at[step - 1],
            send_sem=asend.at[level], recv_sem=arecv.at[level],
            device_id=peer(level, step), device_id_type=LOGICAL,
        )

    def level_start(level):
        for step in range(1, levels[level][1]):
            level_copy(level, step).start()

    basis = [field]
    moments = [sum_all(field * field)]
    state = jnp.concatenate([trace_high + trace_low, field], axis=0)
    mine = None
    for it in range(ITERS):
        last = it + 1 == ITERS
        first = FACES if last else 0
        image = image_of(state[first:], field_high, field_low, first)
        near_raw, own_raw = raw[:, :cols], raw[:, cols:]
        if it:
            mine = mapped(turned(near_raw, near_codes, turn_table), near_kinds, forward)
        for k in range(4):
            guarded(k ^ 1, xcopies[it][k].wait_recv)
        filler = jnp.zeros((ROWS - WIDTH, cols), F32)
        near_got = jnp.concatenate([xbuf[it, k ^ 1, :ROWS] for k in range(4)], axis=1)
        own_got = jnp.concatenate([xbuf[it, k, WIDTH : 2 * WIDTH] for k in range(4)], axis=1)
        own_got = jnp.concatenate([own_got, filler], axis=0)
        if it == 0:
            info = [
                jnp.concatenate([xbuf[it, k, 2 * WIDTH + i : 2 * WIDTH + i + 1] for k in range(4)], axis=1)
                for i in range(3)
            ]
            near_kinds = info[0].astype(jnp.int32)
            near_codes = info[1].astype(jnp.int32)
            diag[:, :cols] = face_mass * info[2]
            mine = mapped(turned(near_raw, near_codes, turn_table), near_kinds, forward)
        theirs = mapped(turned(near_got, own_codes, turn_table), own_kinds, forward)
        jump = own_raw - theirs
        own_flux = diag[:, cols:] * jump
        if last:
            moments.append(sum_all(field * image) + sum_all(own_flux * jump))
            lane_row = lax.broadcasted_iota(jnp.int32, (1, 128), 1)
            row = jnp.zeros((1, 128), F32)
            for i, part in enumerate(moments):
                row = jnp.where(lane_row == i, part, row)
            asrc[0] = row
            level_start(0)
        near_flux = diag[:, :cols] * (mine - own_got)
        near_flux = turned(mapped(near_flux, near_kinds, backward), near_codes, back_table)
        flux = jnp.concatenate([near_flux, own_flux], axis=1)
        parts = []
        for part in split(flux):
            for f in range(6):
                for half in range(ROWS // 16):
                    parts.append(part[half * 16 : (half + 1) * 16] * marks[f])
        faces = dot(jnp.concatenate(parts, axis=0), cells_t[...])
        faces = faces[:FACES] + faces[FACES:]
        both = dot(lift_ref[first:], jnp.concatenate(split(faces), axis=1))
        new = image + both[:, :count] + both[:, count:]
        if last:
            basis.append(new)
            break
        state = new
        trace = state[:FACES]
        trace_high, trace_low = high_low(trace)
        raw = gather(trace_high, trace_low)
        send_out(it + 1, raw)
        field = state[FACES:]
        field_high, field_low = split(field)
        moments.append(sum_all(basis[-1] * field))
        moments.append(sum_all(field * field))
        basis.append(field)

    for level in range(len(levels)):
        landed = slots_refs[level]
        pltpu.make_async_copy(landed, landed, arecv.at[level]).wait()
        value = asrc[level] + jnp.sum(landed[...], axis=0)
        if level + 1 < len(levels):
            asrc[level + 1] = value
            level_start(level + 1)
    value = jnp.broadcast_to(value, (8, 128))
    coefs = conjugate([jnp.broadcast_to(value[:, i : i + 1], (8, count)) for i in range(MOMENTS)])
    cubes = [v[: WIDTH * 8].reshape(WIDTH, 8, count) for v in basis]
    x = coefs[0] * cubes[0]
    r = cubes[0] - coefs[0] * cubes[1]
    for i in range(1, ITERS):
        x = x + coefs[i] * cubes[i]
        r = r - coefs[i] * cubes[i + 1]
    x_out[...] = (UNIT * x)[:, :NODES]
    r_out[...] = r[:, :NODES]

    for copies in xcopies:
        for k in range(4):
            guarded(k, copies[k].wait_send)
    for level in range(len(levels)):
        landed = slots_refs[level]
        pltpu.make_async_copy(landed, landed, asend.at[level]).wait()


def store(x_ref, r_ref, x_hbm, r_hbm, sems):
    copies = [pltpu.make_async_copy(x_ref, x_hbm, sems.at[0]), pltpu.make_async_copy(r_ref, r_hbm, sems.at[1])]
    for copy in copies:
        copy.start()
    for copy in copies:
        copy.wait()


def body(n_sfc, n_grp, right_side, cell_level, own_slot, near_slot, face_kind, orientation, penalty, send_slots, maps):
    count = right_side.shape[-1]
    ghost = send_slots.shape[0] // 4
    pad = -(-ghost // 128) * 128
    levels = ring_levels(n_sfc * n_grp)
    dma = pltpu.SemaphoreType.DMA
    shape = jax.ShapeDtypeStruct((WIDTH, NODES, count), F32)
    operands = (
        right_side.reshape(WIDTH, NODES, count),
        cell_level, own_slot, near_slot, face_kind, orientation, penalty, send_slots,
        jnp.swapaxes(maps, 0, 1), *constants(),
    )
    vmem = pl.BlockSpec(memory_space=pltpu.VMEM)
    hbm = pl.BlockSpec(memory_space=pltpu.HBM)
    operands = [pltpu.with_memory_space_constraint(operand, pltpu.HBM) for operand in operands]
    x, r = pl.pallas_call(
        functools.partial(kernel, (n_sfc, n_grp, count, ghost, pad)),
        out_shape=(pltpu.VMEM(shape.shape, F32),) * 2,
        in_specs=[hbm] * len(operands),
        out_specs=(vmem, vmem),
        scratch_shapes=[pltpu.VMEM(operand.shape, operand.dtype) for operand in operands]
        + [
            pltpu.VMEM((2 * count, 8 * pad), BF16),
            pltpu.VMEM((8 * pad, count), BF16),
            pltpu.VMEM((6, 16, 8 * pad), BF16),
            pltpu.VMEM((4 * ROWS, 128), F32),
            pltpu.VMEM((ROWS, 8 * pad), F32),
            pltpu.VMEM((ITERS, 4, MESSAGE, pad), F32),
            pltpu.VMEM((ITERS, 4, MESSAGE, pad), F32),
            pltpu.VMEM((len(levels), 1, 128), F32),
        ]
        + [pltpu.VMEM((size - 1, 1, 128), F32) for _, size in levels]
        + [
            dma((len(operands),)),
            dma((ITERS, 4)),
            dma((ITERS, 4)),
            dma((len(levels),)),
            dma((len(levels),)),
        ],
        compiler_params=pltpu.CompilerParams(
            collective_id=0, has_side_effects=True, vmem_limit_bytes=16 * 1024 * 1024
        ),
    )(*operands)
    x, r = pl.pallas_call(
        store,
        out_shape=(shape, shape),
        in_specs=[vmem] * 2,
        out_specs=(hbm, hbm),
        scratch_shapes=[dma((2,))],
        compiler_params=pltpu.CompilerParams(vmem_limit_bytes=1024 * 1024),
    )(pltpu.with_memory_space_constraint(x, pltpu.VMEM), pltpu.with_memory_space_constraint(r, pltpu.VMEM))
    return x.reshape(right_side.shape), r.reshape(right_side.shape)


def solution(mesh):
    split_spec = P(("sfc", "grp"))
    field_spec = P(None, None, None, ("sfc", "grp"))
    return jax.shard_map(
        functools.partial(body, mesh.shape["sfc"], mesh.shape["grp"]),
        mesh=mesh,
        in_specs=(field_spec,) + (split_spec,) * 7 + (P(),),
        out_specs=(field_spec, field_spec),
        check_vma=False,
    )
```

```python
import functools

import jax
import jax.numpy as jnp
import numpy as np
from jax import lax
from jax.experimental import pallas as pl
from jax.experimental.pallas import tpu as pltpu
from jax.sharding import PartitionSpec as P

NODES = 5
WIDTH = NODES * NODES
ROWS = 32
FACES = 6 * ROWS
CUBE = 208
ITERS = 3
REACH = 4
MOMENTS = 2 * ITERS
MESSAGE = 56
UNIT = 2.0**-12
OFFSETS = (1, -1, 2, -2)
MASS = 1.0
LOGICAL = pl.DeviceIdType.LOGICAL
F32 = jnp.float32
BF16 = jnp.bfloat16


def node_tables():
    points = np.array([-1.0, -np.sqrt(3.0 / 7.0), 0.0, np.sqrt(3.0 / 7.0), 1.0])
    weights = np.array([0.1, 49.0 / 90.0, 32.0 / 45.0, 49.0 / 90.0, 0.1])
    identity = np.eye(5)
    spacing = points[:, None] - points[None, :] + identity
    barycentric = 1.0 / np.prod(spacing, axis=1)
    offdiag = barycentric[None, :] / barycentric[:, None] / spacing
    diagonal = np.sum(1.0 / spacing, axis=1) - 1.0
    derivs = np.where(identity > 0.5, diagonal[:, None], offdiag)
    return derivs.T @ (weights[:, None] * derivs), weights


def constants():
    stiff, w = node_tables()
    mass = np.diag(w)
    kron = lambda a, b, c: np.kron(np.kron(a, b), c)
    spots = (np.arange(WIDTH)[:, None] * 8 + np.arange(NODES)).reshape(-1)
    nodes = spots.reshape(5, 5, 5)
    layers = [nodes[0], nodes[4], nodes[:, 0], nodes[:, 4], nodes[:, :, 0], nodes[:, :, 4]]
    select = np.zeros((FACES, CUBE))
    for face, layer in enumerate(layers):
        select[face * ROWS + np.arange(WIDTH), layer.reshape(-1)] = 1.0
    both = np.concatenate([select, np.eye(CUBE)])
    volume = np.zeros((CUBE, CUBE))
    volume[np.ix_(spots, spots)] = kron(stiff, mass, mass) + kron(mass, stiff, mass) + kron(mass, mass, stiff)
    volume = both @ volume * UNIT
    high = volume.astype(jnp.bfloat16)
    low = (volume - high.astype(np.float64)).astype(jnp.bfloat16)
    volume = np.concatenate([high, low])
    lift = both @ select.T
    turn = np.zeros((8, ROWS, ROWS))
    for code in range(8):
        order = np.arange(WIDTH).reshape(5, 5)
        order = order[::-1] if code & 1 else order
        order = order[:, ::-1] if code & 2 else order
        order = order.T if code & 4 else order
        turn[code, np.arange(WIDTH), order.reshape(-1)] = 1.0
    back = np.swapaxes(turn, 1, 2)
    turns = np.concatenate([np.concatenate([m, m], axis=2).reshape(8 * ROWS, 2 * ROWS) for m in (turn, back)])
    face_mass = np.zeros((ROWS, 128))
    face_mass[:WIDTH] = UNIT * np.outer(w, w).reshape(-1, 1)
    cube_mass = np.zeros((CUBE, 128))
    cube_mass[spots] = UNIT * MASS * np.einsum("a,b,c->abc", w, w, w).reshape(-1, 1)
    bf = lambda a: jnp.asarray(np.asarray(a, np.float32), BF16)
    return (
        bf(select),
        bf(turns),
        jnp.asarray(np.concatenate([face_mass, both @ cube_mass]), F32),
        bf(volume),
        bf(lift),
    )


def high_low(x):
    high = x.astype(BF16).astype(F32)
    return high, x - high


def split(x):
    high = x.astype(BF16)
    return high, (x - high.astype(F32)).astype(BF16)


def dot(a, b):
    return jnp.dot(a, b, preferred_element_type=F32)


def dot_nt(a, b):
    return lax.dot_general(a, b, (((1,), (1,)), ((), ())), preferred_element_type=F32)


def ring_levels(total):
    levels, stride = [], 1
    while stride < total:
        rest = total // stride
        size = max(g for g in range(1, 33) if rest % g == 0)
        size = rest if size == 1 else size
        levels.append((stride, size))
        stride *= size
    return levels


def conjugate(m):
    def inner(a, b, shift):
        total = None
        for power in range(len(a) + len(b) - 1):
            weight = sum(a[i] * b[power - i] for i in range(len(a)) if 0 <= power - i < len(b))
            term = weight * m[power + shift]
            total = term if total is None else total + term
        return total

    one = jnp.ones_like(m[0])
    x, r, p = [], [one], [one]
    norm = m[0]
    for it in range(ITERS):
        alpha = norm / inner(p, p, 1)
        x = [(x[i] if i < len(x) else 0.0) + alpha * p[i] for i in range(len(p))]
        r = [one] + [-value for value in x]
        if it + 1 < ITERS:
            new = inner(r, r, 0)
            beta = new / norm
            p = [r[i] + (beta * p[i] if i < len(p) else 0.0) for i in range(len(r))]
            norm = new
    return x


def kernel(
    dims,
    rhs_hbm, level_hbm, own_hbm, near_hbm, kind_hbm, orient_hbm, pen_hbm, send_hbm, maps_hbm,
    sel_hbm, turn_hbm, mass_hbm, vol_hbm, lift_hbm,
    x_out, r_out,
    rhs_ref, level_ref, own_ref, near_ref, kind_ref, orient_ref, pen_ref, send_ref, maps_ref,
    sel_ref, turn_ref, mass_ref, vol_ref, lift_ref,
    cells, cells_t, marks, mapz, diag, xsrc, xbuf, asrc, *rest,
):
    n_sfc, n_grp, count, ghost, pad = dims
    total = n_sfc * n_grp
    levels = ring_levels(total)
    slots_refs = rest[: len(levels)]
    insem, xsend, xrecv, asend, arecv, *relay = rest[len(levels):]
    me = lax.axis_index("sfc") * n_grp + lax.axis_index("grp")
    slots = 6 * count
    entries = 4 * ghost
    cols = 4 * pad

    loads = {}
    for i, (name, src, dst) in enumerate([
        ("near", near_hbm, near_ref), ("own", own_hbm, own_ref), ("send", send_hbm, send_ref),
        ("level", level_hbm, level_ref), ("rhs", rhs_hbm, rhs_ref), ("sel", sel_hbm, sel_ref),
        ("kind", kind_hbm, kind_ref), ("orient", orient_hbm, orient_ref), ("pen", pen_hbm, pen_ref),
        ("turn", turn_hbm, turn_ref), ("mass", mass_hbm, mass_ref), ("maps", maps_hbm, maps_ref),
        ("vol", vol_hbm, vol_ref), ("lift", lift_hbm, lift_ref),
    ]):
        loads[name] = pltpu.make_async_copy(src, dst, insem.at[i])
        loads[name].start()

    exists = [(me + offset >= 0) & (me + offset < total) for offset in OFFSETS]

    def near_device(k):
        offset = OFFSETS[k]
        return me + jnp.where(exists[k], offset, offset - total if offset > 0 else offset + total)

    digits = [lax.rem(me // stride, size) for stride, size in levels]

    def peer(level, step):
        stride, size = levels[level]
        return me + jnp.where(digits[level] + step >= size, step - size, step) * stride

    def guarded(k, action):
        @pl.when(exists[k])
        def _():
            action()

    barrier = pltpu.get_barrier_semaphore()
    relayed = len(levels) == 1 and REACH << ITERS == total
    greeted = 0

    def reach(distance, action):
        for offset in (distance, -distance):
            action(me + jnp.where((me + offset >= 0) & (me + offset < total), offset, offset - total if offset > 0 else offset + total))

    if relayed:
        for distance in range(1, REACH + 1):
            reach(distance, lambda device: pl.semaphore_signal(barrier, inc=1, device_id=device, device_id_type=LOGICAL))
        greeted = 2 * REACH
    else:
        for level, (_, size) in enumerate(levels):
            for step in range(1, size):
                pl.semaphore_signal(barrier, inc=1, device_id=peer(level, step), device_id_type=LOGICAL)
            greeted += size - 1
        for k in range(4):
            pl.semaphore_signal(barrier, inc=1, device_id=near_device(k), device_id_type=LOGICAL)
        greeted += 4

    def relay_send(turn_number):
        if relayed:
            reach(REACH << turn_number, lambda device: pl.semaphore_signal(
                relay[turn_number], inc=1, device_id=device, device_id_type=LOGICAL))

    def relay_wait(turn_number):
        if relayed:
            pl.semaphore_wait(relay[turn_number], 2)

    for k in range(4):
        @pl.when(jnp.logical_not(exists[k]))
        def _(k=k):
            for it in range(ITERS):
                xbuf[it, k] = jnp.zeros(xbuf.shape[2:], F32)

    for name in ("near", "own", "send", "level", "rhs", "sel", "kind", "orient", "pen"):
        loads[name].wait()
    line = lambda ref: ref[...].reshape(1, -1)

    inner = lax.broadcasted_iota(jnp.int32, (WIDTH, 8, count), 1) < NODES
    padded = jnp.concatenate([rhs_ref[...], jnp.zeros((WIDTH, 8 - NODES, count), F32)], axis=1)
    field = jnp.concatenate(
        [jnp.where(inner, padded, 0.0).reshape(WIDTH * 8, count), jnp.zeros((CUBE - WIDTH * 8, count), F32)], axis=0
    )
    field_high, field_low = split(field)
    picked = dot(sel_ref[...], jnp.concatenate([field_high, field_low], axis=1))
    scale = jnp.exp2(-line(level_ref).astype(F32))
    face_row = lax.rem(lax.broadcasted_iota(jnp.int32, (FACES, count), 0), ROWS)
    trace_high = jnp.where(face_row == WIDTH, scale, picked[:, :count])
    trace_low = picked[:, count:]

    own = line(own_ref)
    pen = line(pen_ref)
    pen_a, pen_b = high_low(pen)
    pen_b, pen_c = high_low(pen_b)
    send = line(send_ref)
    zero_row = jnp.zeros_like(pen)
    rows = [(own >> 8).astype(F32), (own & 255).astype(F32), line(kind_ref).astype(F32), line(orient_ref).astype(F32)]
    params = jnp.concatenate(rows + [pen_a, pen_b, pen_c, zero_row], axis=0).astype(BF16)
    sent_rows = jnp.concatenate([(send >> 8).astype(F32), (send & 255).astype(F32)] + [zero_row] * 6, axis=0).astype(BF16)
    near = jnp.broadcast_to(line(near_ref), (pad, entries))
    spot = lax.broadcasted_iota(jnp.int32, (pad, entries), 0)
    lane = lax.broadcasted_iota(jnp.int32, (pad, entries), 1)
    inside = spot < ghost
    order, spread = [], []
    for k in range(4):
        order.append(jnp.where(inside & (near == spot + (slots + k * ghost)), 1.0, 0.0).astype(BF16))
        spread.append(jnp.where(inside & (lane == spot + k * ghost), 1.0, 0.0).astype(BF16))
    ordered = dot_nt(params, jnp.concatenate(order, axis=0))
    spread = dot_nt(sent_rows, jnp.concatenate(spread, axis=0))
    slot = jnp.concatenate(
        [spread[0:1] * 256.0 + spread[1:2], ordered[0:1] * 256.0 + ordered[1:2]], axis=1
    ).astype(jnp.int32)
    face = jnp.zeros_like(slot)
    for f in range(1, 6):
        face = face + jnp.where(slot >= f * count, 1, 0)
    cell = slot - face * count
    cell_row = lax.broadcasted_iota(jnp.int32, (count, 2 * cols), 0)
    chosen = jnp.where(cell_row == cell, 1.0, 0.0)
    cells[:count] = chosen.astype(BF16)
    cells[count:] = chosen.astype(BF16)

    def gather(high, low):
        found = dot(jnp.concatenate([high, low], axis=1).astype(BF16), cells[...])
        raw = found[:ROWS]
        for f in range(1, 6):
            raw = jnp.where(face == f, found[f * ROWS : (f + 1) * ROWS], raw)
        return raw

    raw = gather(trace_high, trace_low)
    strength = (ordered[4:5] + ordered[5:6] + ordered[6:7]) * raw[WIDTH : WIDTH + 1, cols:]
    sub = lax.broadcasted_iota(jnp.int32, (8, cols), 0)
    tail = jnp.where(sub == 0, ordered[2:3], jnp.where(sub == 1, ordered[3:4], jnp.where(sub == 2, strength, 0.0)))

    pl.semaphore_wait(barrier, greeted)

    xcopies = []

    def send_out(turn_number, raw):
        count_rows = MESSAGE if turn_number == 0 else 2 * WIDTH
        copies = []
        for k in range(4):
            other = cols + (k ^ 1) * pad
            xsrc[turn_number, k, :WIDTH] = raw[:WIDTH, k * pad : (k + 1) * pad]
            xsrc[turn_number, k, WIDTH : 2 * WIDTH] = raw[:WIDTH, other : other + pad]
            if turn_number == 0:
                xsrc[turn_number, k, 2 * WIDTH :] = tail[: MESSAGE - 2 * WIDTH, other - cols : other - cols + pad]
            copies.append(pltpu.make_async_remote_copy(
                src_ref=xsrc.at[turn_number, k, pl.ds(0, count_rows)],
                dst_ref=xbuf.at[turn_number, k ^ 1, pl.ds(0, count_rows)],
                send_sem=xsend.at[turn_number, k], recv_sem=xrecv.at[turn_number, k ^ 1],
                device_id=near_device(k), device_id_type=LOGICAL,
            ))
        for k in (2, 3, 0, 1):
            guarded(k, copies[k].start)
        xcopies.append(copies)
        relay_send(turn_number)

    send_out(0, raw)

    for name in ("turn", "mass", "maps", "vol", "lift"):
        loads[name].wait()
    for f in range(6):
        marks[f] = jnp.broadcast_to(jnp.where(face == f, 1.0, 0.0), (16, 2 * cols)).astype(BF16)
    cells_t[...] = chosen.T.astype(BF16)
    mapz[...] = jnp.zeros_like(mapz)
    for s in range(4):
        mapz[s * ROWS : s * ROWS + WIDTH, 0:WIDTH] = maps_ref[:, s, :]
    maps = mapz[...]
    transposed = maps.T
    backs = jnp.concatenate([transposed[:ROWS, s * ROWS : (s + 1) * ROWS] for s in range(4)], axis=0)

    def three(matrix):
        high, low = split(matrix)
        return jnp.concatenate([high, high, low], axis=1)

    forward = three(maps[:, :ROWS])
    backward = three(backs)
    face_mass = jnp.concatenate([mass_ref[:ROWS]] * (cols // 128), axis=1)
    diag[:, cols:] = face_mass * strength
    mass_scale = mass_ref[ROWS:] * (scale * scale * scale)

    def turned(values, codes, table):
        forms = dot(table, jnp.concatenate(split(values), axis=0))
        result = forms[:ROWS]
        for code in range(1, 8):
            result = jnp.where(codes == code, forms[code * ROWS : (code + 1) * ROWS], result)
        return result

    def mapped(values, kinds, table):
        high, low = split(values)
        forms = dot(table, jnp.concatenate([high, low, high], axis=0))
        result = jnp.where(kinds == 1, values, 0.0)
        for s in range(4):
            result = jnp.where(kinds == s + 2, forms[s * ROWS : (s + 1) * ROWS], result)
        return result

    turn_table = turn_ref[: 8 * ROWS]
    back_table = turn_ref[8 * ROWS :]
    own_kinds = ordered[2:3].astype(jnp.int32)
    own_codes = ordered[3:4].astype(jnp.int32)

    def image_of(state, high, low, first):
        both = dot(vol_ref[first : FACES + CUBE], jnp.concatenate([high, low], axis=1))
        both = both[:, :count] + both[:, count:] + dot(vol_ref[FACES + CUBE + first :], high)
        return both * scale + mass_scale[first:] * state

    def sum_all(a):
        return jnp.sum(jnp.sum(a, axis=0, keepdims=True), axis=1, keepdims=True)

    def level_copy(level, step):
        return pltpu.make_async_remote_copy(
            src_ref=asrc.at[level], dst_ref=slots_refs[level].at[step - 1],
            send_sem=asend.at[level], recv_sem=arecv.at[level],
            device_id=peer(level, step), device_id_type=LOGICAL,
        )

    def level_start(level):
        for step in range(1, levels[level][1]):
            level_copy(level, step).start()

    basis = [field]
    moments = [sum_all(field * field)]
    state = jnp.concatenate([trace_high + trace_low, field], axis=0)
    mine = None
    for it in range(ITERS):
        last = it + 1 == ITERS
        first = FACES if last else 0
        image = image_of(state[first:], field_high, field_low, first)
        near_raw, own_raw = raw[:, :cols], raw[:, cols:]
        if it:
            mine = mapped(turned(near_raw, near_codes, turn_table), near_kinds, forward)
        for k in range(4):
            guarded(k ^ 1, xcopies[it][k].wait_recv)
        relay_wait(it)
        filler = jnp.zeros((ROWS - WIDTH, cols), F32)
        near_got = jnp.concatenate([xbuf[it, k ^ 1, :ROWS] for k in range(4)], axis=1)
        own_got = jnp.concatenate([xbuf[it, k, WIDTH : 2 * WIDTH] for k in range(4)], axis=1)
        own_got = jnp.concatenate([own_got, filler], axis=0)
        if it == 0:
            info = [
                jnp.concatenate([xbuf[it, k, 2 * WIDTH + i : 2 * WIDTH + i + 1] for k in range(4)], axis=1)
                for i in range(3)
            ]
            near_kinds = info[0].astype(jnp.int32)
            near_codes = info[1].astype(jnp.int32)
            diag[:, :cols] = face_mass * info[2]
            mine = mapped(turned(near_raw, near_codes, turn_table), near_kinds, forward)
        theirs = mapped(turned(near_got, own_codes, turn_table), own_kinds, forward)
        jump = own_raw - theirs
        own_flux = diag[:, cols:] * jump
        if last:
            moments.append(sum_all(field * image) + sum_all(own_flux * jump))
            lane_row = lax.broadcasted_iota(jnp.int32, (1, 128), 1)
            row = jnp.zeros((1, 128), F32)
            for i, part in enumerate(moments):
                row = jnp.where(lane_row == i, part, row)
            asrc[0] = row
            level_start(0)
        near_flux = diag[:, :cols] * (mine - own_got)
        near_flux = turned(mapped(near_flux, near_kinds, backward), near_codes, back_table)
        flux = jnp.concatenate([near_flux, own_flux], axis=1)
        parts = []
        for part in split(flux):
            for f in range(6):
                for half in range(ROWS // 16):
                    parts.append(part[half * 16 : (half + 1) * 16] * marks[f])
        faces = dot(jnp.concatenate(parts, axis=0), cells_t[...])
        faces = faces[:FACES] + faces[FACES:]
        both = dot(lift_ref[first:], jnp.concatenate(split(faces), axis=1))
        new = image + both[:, :count] + both[:, count:]
        if last:
            basis.append(new)
            break
        state = new
        trace = state[:FACES]
        trace_high, trace_low = high_low(trace)
        raw = gather(trace_high, trace_low)
        send_out(it + 1, raw)
        field = state[FACES:]
        field_high, field_low = split(field)
        moments.append(sum_all(basis[-1] * field))
        moments.append(sum_all(field * field))
        basis.append(field)

    for level in range(len(levels)):
        landed = slots_refs[level]
        pltpu.make_async_copy(landed, landed, arecv.at[level]).wait()
        value = asrc[level] + jnp.sum(landed[...], axis=0)
        if level + 1 < len(levels):
            asrc[level + 1] = value
            level_start(level + 1)
    value = jnp.broadcast_to(value, (8, 128))
    coefs = conjugate([jnp.broadcast_to(value[:, i : i + 1], (8, count)) for i in range(MOMENTS)])
    cubes = [v[: WIDTH * 8].reshape(WIDTH, 8, count) for v in basis]
    x = coefs[0] * cubes[0]
    r = cubes[0] - coefs[0] * cubes[1]
    for i in range(1, ITERS):
        x = x + coefs[i] * cubes[i]
        r = r - coefs[i] * cubes[i + 1]
    x_out[...] = (UNIT * x)[:, :NODES]
    r_out[...] = r[:, :NODES]

    for copies in xcopies:
        for k in range(4):
            guarded(k, copies[k].wait_send)
    for level in range(len(levels)):
        landed = slots_refs[level]
        pltpu.make_async_copy(landed, landed, asend.at[level]).wait()


def store(x_ref, r_ref, x_hbm, r_hbm, sems):
    copies = [pltpu.make_async_copy(x_ref, x_hbm, sems.at[0]), pltpu.make_async_copy(r_ref, r_hbm, sems.at[1])]
    for copy in copies:
        copy.start()
    for copy in copies:
        copy.wait()


def body(n_sfc, n_grp, right_side, cell_level, own_slot, near_slot, face_kind, orientation, penalty, send_slots, maps):
    count = right_side.shape[-1]
    ghost = send_slots.shape[0] // 4
    pad = -(-ghost // 128) * 128
    levels = ring_levels(n_sfc * n_grp)
    dma = pltpu.SemaphoreType.DMA
    shape = jax.ShapeDtypeStruct((WIDTH, NODES, count), F32)
    operands = (
        right_side.reshape(WIDTH, NODES, count),
        cell_level, own_slot, near_slot, face_kind, orientation, penalty, send_slots,
        jnp.swapaxes(maps, 0, 1), *constants(),
    )
    vmem = pl.BlockSpec(memory_space=pltpu.VMEM)
    hbm = pl.BlockSpec(memory_space=pltpu.HBM)
    operands = [pltpu.with_memory_space_constraint(operand, pltpu.HBM) for operand in operands]
    x, r = pl.pallas_call(
        functools.partial(kernel, (n_sfc, n_grp, count, ghost, pad)),
        out_shape=(pltpu.VMEM(shape.shape, F32),) * 2,
        in_specs=[hbm] * len(operands),
        out_specs=(vmem, vmem),
        scratch_shapes=[pltpu.VMEM(operand.shape, operand.dtype) for operand in operands]
        + [
            pltpu.VMEM((2 * count, 8 * pad), BF16),
            pltpu.VMEM((8 * pad, count), BF16),
            pltpu.VMEM((6, 16, 8 * pad), BF16),
            pltpu.VMEM((4 * ROWS, 128), F32),
            pltpu.VMEM((ROWS, 8 * pad), F32),
            pltpu.VMEM((ITERS, 4, MESSAGE, pad), F32),
            pltpu.VMEM((ITERS, 4, MESSAGE, pad), F32),
            pltpu.VMEM((len(levels), 1, 128), F32),
        ]
        + [pltpu.VMEM((size - 1, 1, 128), F32) for _, size in levels]
        + [
            dma((len(operands),)),
            dma((ITERS, 4)),
            dma((ITERS, 4)),
            dma((len(levels),)),
            dma((len(levels),)),
        ]
        + [pltpu.SemaphoreType.REGULAR] * ITERS,
        compiler_params=pltpu.CompilerParams(
            collective_id=0, has_side_effects=True, vmem_limit_bytes=16 * 1024 * 1024
        ),
    )(*operands)
    x, r = pl.pallas_call(
        store,
        out_shape=(shape, shape),
        in_specs=[vmem] * 2,
        out_specs=(hbm, hbm),
        scratch_shapes=[dma((2,))],
        compiler_params=pltpu.CompilerParams(vmem_limit_bytes=1024 * 1024),
    )(pltpu.with_memory_space_constraint(x, pltpu.VMEM), pltpu.with_memory_space_constraint(r, pltpu.VMEM))
    return x.reshape(right_side.shape), r.reshape(right_side.shape)


def solution(mesh):
    split_spec = P(("sfc", "grp"))
    field_spec = P(None, None, None, ("sfc", "grp"))
    return jax.shard_map(
        functools.partial(body, mesh.shape["sfc"], mesh.shape["grp"]),
        mesh=mesh,
        in_specs=(field_spec,) + (split_spec,) * 7 + (P(),),
        out_specs=(field_spec, field_spec),
        check_vma=False,
    )
```

```python
import functools

import jax
import jax.numpy as jnp
import numpy as np
from jax import lax
from jax.experimental import pallas as pl
from jax.experimental.pallas import tpu as pltpu
from jax.sharding import PartitionSpec as P

NODES = 5
WIDTH = NODES * NODES
ROWS = 32
FACES = 6 * ROWS
CUBE = 208
ITERS = 3
REACH = 4
MOMENTS = 2 * ITERS
MESSAGE = 56
UNIT = 2.0**-12
OFFSETS = (1, -1, 2, -2)
MASS = 1.0
LOGICAL = pl.DeviceIdType.LOGICAL
F32 = jnp.float32
BF16 = jnp.bfloat16


def node_tables():
    points = np.array([-1.0, -np.sqrt(3.0 / 7.0), 0.0, np.sqrt(3.0 / 7.0), 1.0])
    weights = np.array([0.1, 49.0 / 90.0, 32.0 / 45.0, 49.0 / 90.0, 0.1])
    identity = np.eye(5)
    spacing = points[:, None] - points[None, :] + identity
    barycentric = 1.0 / np.prod(spacing, axis=1)
    offdiag = barycentric[None, :] / barycentric[:, None] / spacing
    diagonal = np.sum(1.0 / spacing, axis=1) - 1.0
    derivs = np.where(identity > 0.5, diagonal[:, None], offdiag)
    return derivs.T @ (weights[:, None] * derivs), weights


def constants():
    stiff, w = node_tables()
    mass = np.diag(w)
    kron = lambda a, b, c: np.kron(np.kron(a, b), c)
    spots = (np.arange(WIDTH)[:, None] * 8 + np.arange(NODES)).reshape(-1)
    nodes = spots.reshape(5, 5, 5)
    layers = [nodes[0], nodes[4], nodes[:, 0], nodes[:, 4], nodes[:, :, 0], nodes[:, :, 4]]
    select = np.zeros((FACES, CUBE))
    for face, layer in enumerate(layers):
        select[face * ROWS + np.arange(WIDTH), layer.reshape(-1)] = 1.0
    both = np.concatenate([select, np.eye(CUBE)])
    volume = np.zeros((CUBE, CUBE))
    volume[np.ix_(spots, spots)] = kron(stiff, mass, mass) + kron(mass, stiff, mass) + kron(mass, mass, stiff)
    volume = both @ volume * UNIT
    high = volume.astype(jnp.bfloat16)
    low = (volume - high.astype(np.float64)).astype(jnp.bfloat16)
    volume = np.concatenate([high, low])
    lift = both @ select.T
    turn = np.zeros((8, ROWS, ROWS))
    for code in range(8):
        order = np.arange(WIDTH).reshape(5, 5)
        order = order[::-1] if code & 1 else order
        order = order[:, ::-1] if code & 2 else order
        order = order.T if code & 4 else order
        turn[code, np.arange(WIDTH), order.reshape(-1)] = 1.0
    back = np.swapaxes(turn, 1, 2)
    turns = np.concatenate([np.concatenate([m, m], axis=2).reshape(8 * ROWS, 2 * ROWS) for m in (turn, back)])
    face_mass = np.zeros((ROWS, 128))
    face_mass[:WIDTH] = UNIT * np.outer(w, w).reshape(-1, 1)
    cube_mass = np.zeros((CUBE, 128))
    cube_mass[spots] = UNIT * MASS * np.einsum("a,b,c->abc", w, w, w).reshape(-1, 1)
    bf = lambda a: jnp.asarray(np.asarray(a, np.float32), BF16)
    return (
        bf(select),
        bf(turns),
        jnp.asarray(np.concatenate([face_mass, both @ cube_mass]), F32),
        bf(volume),
        bf(lift),
    )


def high_low(x):
    high = x.astype(BF16).astype(F32)
    return high, x - high


def split(x):
    high = x.astype(BF16)
    return high, (x - high.astype(F32)).astype(BF16)


def dot(a, b):
    return jnp.dot(a, b, preferred_element_type=F32)


def dot_nt(a, b):
    return lax.dot_general(a, b, (((1,), (1,)), ((), ())), preferred_element_type=F32)


def ring_levels(total):
    levels, stride = [], 1
    while stride < total:
        rest = total // stride
        size = max(g for g in range(1, 33) if rest % g == 0)
        size = rest if size == 1 else size
        levels.append((stride, size))
        stride *= size
    return levels


def conjugate(m):
    def inner(a, b, shift):
        total = None
        for power in range(len(a) + len(b) - 1):
            weight = sum(a[i] * b[power - i] for i in range(len(a)) if 0 <= power - i < len(b))
            term = weight * m[power + shift]
            total = term if total is None else total + term
        return total

    one = jnp.ones_like(m[0])
    x, r, p = [], [one], [one]
    norm = m[0]
    for it in range(ITERS):
        alpha = norm / inner(p, p, 1)
        x = [(x[i] if i < len(x) else 0.0) + alpha * p[i] for i in range(len(p))]
        r = [one] + [-value for value in x]
        if it + 1 < ITERS:
            new = inner(r, r, 0)
            beta = new / norm
            p = [r[i] + (beta * p[i] if i < len(p) else 0.0) for i in range(len(r))]
            norm = new
    return x


def kernel(
    dims,
    rhs_hbm, level_hbm, own_hbm, near_hbm, kind_hbm, orient_hbm, pen_hbm, send_hbm, maps_hbm,
    sel_hbm, turn_hbm, mass_hbm, vol_hbm, lift_hbm,
    x_out, r_out,
    rhs_ref, level_ref, own_ref, near_ref, kind_ref, orient_ref, pen_ref, send_ref, maps_ref,
    sel_ref, turn_ref, mass_ref, vol_ref, lift_ref,
    cells, cells_t, marks, mapz, diag, xsrc, xbuf, asrc, *rest,
):
    n_sfc, n_grp, count, ghost, pad = dims
    total = n_sfc * n_grp
    levels = ring_levels(total)
    slots_refs = rest[: len(levels)]
    insem, xsend, xrecv, asend, arecv, *relay = rest[len(levels):]
    me = lax.axis_index("sfc") * n_grp + lax.axis_index("grp")
    slots = 6 * count
    entries = 4 * ghost
    cols = 4 * pad

    loads = {}
    for i, (name, src, dst) in enumerate([
        ("near", near_hbm, near_ref), ("own", own_hbm, own_ref), ("send", send_hbm, send_ref),
        ("level", level_hbm, level_ref), ("rhs", rhs_hbm, rhs_ref), ("sel", sel_hbm, sel_ref),
        ("kind", kind_hbm, kind_ref), ("orient", orient_hbm, orient_ref), ("pen", pen_hbm, pen_ref),
        ("turn", turn_hbm, turn_ref), ("mass", mass_hbm, mass_ref), ("maps", maps_hbm, maps_ref),
        ("vol", vol_hbm, vol_ref), ("lift", lift_hbm, lift_ref),
    ]):
        loads[name] = pltpu.make_async_copy(src, dst, insem.at[i])
        loads[name].start()

    exists = [(me + offset >= 0) & (me + offset < total) for offset in OFFSETS]

    def near_device(k):
        offset = OFFSETS[k]
        return me + jnp.where(exists[k], offset, offset - total if offset > 0 else offset + total)

    digits = [lax.rem(me // stride, size) for stride, size in levels]

    def peer(level, step):
        stride, size = levels[level]
        return me + jnp.where(digits[level] + step >= size, step - size, step) * stride

    def guarded(k, action):
        @pl.when(exists[k])
        def _():
            action()

    barrier = pltpu.get_barrier_semaphore()
    relayed = len(levels) == 1 and REACH << ITERS == total
    greeted = 0

    def reach(distance, action):
        for offset in (distance, -distance):
            action(me + jnp.where((me + offset >= 0) & (me + offset < total), offset, offset - total if offset > 0 else offset + total))

    if relayed:
        for distance in range(1, REACH + 1):
            reach(distance, lambda device: pl.semaphore_signal(barrier, inc=1, device_id=device, device_id_type=LOGICAL))
        greeted = 2 * REACH
    else:
        for level, (_, size) in enumerate(levels):
            for step in range(1, size):
                pl.semaphore_signal(barrier, inc=1, device_id=peer(level, step), device_id_type=LOGICAL)
            greeted += size - 1
        for k in range(4):
            pl.semaphore_signal(barrier, inc=1, device_id=near_device(k), device_id_type=LOGICAL)
        greeted += 4

    def relay_send(turn_number):
        if relayed:
            reach(REACH << turn_number, lambda device: pl.semaphore_signal(
                relay[turn_number], inc=1, device_id=device, device_id_type=LOGICAL))

    def relay_wait(turn_number):
        if relayed:
            pl.semaphore_wait(relay[turn_number], 2)

    for k in range(4):
        @pl.when(jnp.logical_not(exists[k]))
        def _(k=k):
            for it in range(ITERS):
                xbuf[it, k] = jnp.zeros(xbuf.shape[2:], F32)

    for name in ("near", "own", "send", "level", "rhs", "sel", "kind", "orient", "pen"):
        loads[name].wait()
    line = lambda ref: ref[...].reshape(1, -1)

    inner = lax.broadcasted_iota(jnp.int32, (WIDTH, 8, count), 1) < NODES
    padded = jnp.concatenate([rhs_ref[...], jnp.zeros((WIDTH, 8 - NODES, count), F32)], axis=1)
    field = jnp.concatenate(
        [jnp.where(inner, padded, 0.0).reshape(WIDTH * 8, count), jnp.zeros((CUBE - WIDTH * 8, count), F32)], axis=0
    )
    field_high, field_low = split(field)
    picked = dot(sel_ref[...], jnp.concatenate([field_high, field_low], axis=1))
    scale = jnp.exp2(-line(level_ref).astype(F32))
    face_row = lax.rem(lax.broadcasted_iota(jnp.int32, (FACES, count), 0), ROWS)
    trace_high = jnp.where(face_row == WIDTH, scale, picked[:, :count])
    trace_low = picked[:, count:]

    own = line(own_ref)
    pen = line(pen_ref)
    pen_a, pen_b = high_low(pen)
    pen_b, pen_c = high_low(pen_b)
    send = line(send_ref)
    zero_row = jnp.zeros_like(pen)
    rows = [(own >> 8).astype(F32), (own & 255).astype(F32), line(kind_ref).astype(F32), line(orient_ref).astype(F32)]
    params = jnp.concatenate(rows + [pen_a, pen_b, pen_c, zero_row], axis=0).astype(BF16)
    sent_rows = jnp.concatenate([(send >> 8).astype(F32), (send & 255).astype(F32)] + [zero_row] * 6, axis=0).astype(BF16)
    near = jnp.broadcast_to(line(near_ref), (pad, entries))
    spot = lax.broadcasted_iota(jnp.int32, (pad, entries), 0)
    lane = lax.broadcasted_iota(jnp.int32, (pad, entries), 1)
    inside = spot < ghost
    order, spread = [], []
    for k in range(4):
        order.append(jnp.where(inside & (near == spot + (slots + k * ghost)), 1.0, 0.0).astype(BF16))
        spread.append(jnp.where(inside & (lane == spot + k * ghost), 1.0, 0.0).astype(BF16))
    ordered = dot_nt(params, jnp.concatenate(order, axis=0))
    spread = dot_nt(sent_rows, jnp.concatenate(spread, axis=0))
    slot = jnp.concatenate(
        [spread[0:1] * 256.0 + spread[1:2], ordered[0:1] * 256.0 + ordered[1:2]], axis=1
    ).astype(jnp.int32)
    face = jnp.zeros_like(slot)
    for f in range(1, 6):
        face = face + jnp.where(slot >= f * count, 1, 0)
    cell = slot - face * count
    cell_row = lax.broadcasted_iota(jnp.int32, (count, 2 * cols), 0)
    chosen = jnp.where(cell_row == cell, 1.0, 0.0)
    cells[:count] = chosen.astype(BF16)
    cells[count:] = chosen.astype(BF16)

    def gather(high, low):
        found = dot(jnp.concatenate([high, low], axis=1).astype(BF16), cells[...])
        raw = found[:ROWS]
        for f in range(1, 6):
            raw = jnp.where(face == f, found[f * ROWS : (f + 1) * ROWS], raw)
        return raw

    raw = gather(trace_high, trace_low)
    strength = (ordered[4:5] + ordered[5:6] + ordered[6:7]) * raw[WIDTH : WIDTH + 1, cols:]
    sub = lax.broadcasted_iota(jnp.int32, (8, cols), 0)
    tail = jnp.where(sub == 0, ordered[2:3], jnp.where(sub == 1, ordered[3:4], jnp.where(sub == 2, strength, 0.0)))

    pl.semaphore_wait(barrier, greeted)

    xcopies = []

    def send_out(turn_number, raw):
        count_rows = MESSAGE if turn_number == 0 else 2 * WIDTH
        copies = []
        for k in range(4):
            other = cols + (k ^ 1) * pad
            xsrc[turn_number, k, :WIDTH] = raw[:WIDTH, k * pad : (k + 1) * pad]
            xsrc[turn_number, k, WIDTH : 2 * WIDTH] = raw[:WIDTH, other : other + pad]
            if turn_number == 0:
                xsrc[turn_number, k, 2 * WIDTH :] = tail[: MESSAGE - 2 * WIDTH, other - cols : other - cols + pad]
            copies.append(pltpu.make_async_remote_copy(
                src_ref=xsrc.at[turn_number, k, pl.ds(0, count_rows)],
                dst_ref=xbuf.at[turn_number, k ^ 1, pl.ds(0, count_rows)],
                send_sem=xsend.at[turn_number, k], recv_sem=xrecv.at[turn_number, k ^ 1],
                device_id=near_device(k), device_id_type=LOGICAL,
            ))
        for k in (2, 3, 0, 1):
            guarded(k, copies[k].start)
        xcopies.append(copies)
        relay_send(turn_number)

    send_out(0, raw)

    for name in ("turn", "mass", "maps", "vol", "lift"):
        loads[name].wait()
    for pair in range(3):
        marks[pair] = jnp.broadcast_to(jnp.where(face >> 1 == pair, 1.0, 0.0), (16, 2 * cols)).astype(BF16)
    for end in range(2):
        cells_t[:, end * count : (end + 1) * count] = jnp.where(face & 1 == end, chosen, 0.0).T.astype(BF16)
    mapz[...] = jnp.zeros_like(mapz)
    for s in range(4):
        mapz[s * ROWS : s * ROWS + WIDTH, 0:WIDTH] = maps_ref[:, s, :]
    maps = mapz[...]
    transposed = maps.T
    backs = jnp.concatenate([transposed[:ROWS, s * ROWS : (s + 1) * ROWS] for s in range(4)], axis=0)

    def three(matrix):
        high, low = split(matrix)
        return jnp.concatenate([high, high, low], axis=1)

    forward = three(maps[:, :ROWS])
    backward = three(backs)
    face_mass = jnp.concatenate([mass_ref[:ROWS]] * (cols // 128), axis=1)
    diag[:, cols:] = face_mass * strength
    mass_scale = mass_ref[ROWS:] * (scale * scale * scale)

    def turned(values, codes, table):
        forms = dot(table, jnp.concatenate(split(values), axis=0))
        result = forms[:ROWS]
        for code in range(1, 8):
            result = jnp.where(codes == code, forms[code * ROWS : (code + 1) * ROWS], result)
        return result

    def mapped(values, kinds, table):
        high, low = split(values)
        forms = dot(table, jnp.concatenate([high, low, high], axis=0))
        result = jnp.where(kinds == 1, values, 0.0)
        for s in range(4):
            result = jnp.where(kinds == s + 2, forms[s * ROWS : (s + 1) * ROWS], result)
        return result

    turn_table = turn_ref[: 8 * ROWS]
    back_table = turn_ref[8 * ROWS :]
    own_kinds = ordered[2:3].astype(jnp.int32)
    own_codes = ordered[3:4].astype(jnp.int32)

    def image_of(state, high, low, first):
        both = dot(vol_ref[first : FACES + CUBE], jnp.concatenate([high, low], axis=1))
        both = both[:, :count] + both[:, count:] + dot(vol_ref[FACES + CUBE + first :], high)
        return both * scale + mass_scale[first:] * state

    def sum_all(a):
        return jnp.sum(jnp.sum(a, axis=0, keepdims=True), axis=1, keepdims=True)

    def level_copy(level, step):
        return pltpu.make_async_remote_copy(
            src_ref=asrc.at[level], dst_ref=slots_refs[level].at[step - 1],
            send_sem=asend.at[level], recv_sem=arecv.at[level],
            device_id=peer(level, step), device_id_type=LOGICAL,
        )

    def level_start(level):
        for step in range(1, levels[level][1]):
            level_copy(level, step).start()

    basis = [field]
    moments = [sum_all(field * field)]
    state = jnp.concatenate([trace_high + trace_low, field], axis=0)
    mine = None
    for it in range(ITERS):
        last = it + 1 == ITERS
        first = FACES if last else 0
        image = image_of(state[first:], field_high, field_low, first)
        near_raw, own_raw = raw[:, :cols], raw[:, cols:]
        if last:
            moments.append(jnp.sum(field * image, axis=0, keepdims=True))
        if it:
            mine = mapped(turned(near_raw, near_codes, turn_table), near_kinds, forward)
        for k in range(4):
            guarded(k ^ 1, xcopies[it][k].wait_recv)
        relay_wait(it)
        filler = jnp.zeros((ROWS - WIDTH, cols), F32)
        near_got = jnp.concatenate([xbuf[it, k ^ 1, :ROWS] for k in range(4)], axis=1)
        own_got = jnp.concatenate([xbuf[it, k, WIDTH : 2 * WIDTH] for k in range(4)], axis=1)
        own_got = jnp.concatenate([own_got, filler], axis=0)
        if it == 0:
            info = [
                jnp.concatenate([xbuf[it, k, 2 * WIDTH + i : 2 * WIDTH + i + 1] for k in range(4)], axis=1)
                for i in range(3)
            ]
            near_kinds = info[0].astype(jnp.int32)
            near_codes = info[1].astype(jnp.int32)
            diag[:, :cols] = face_mass * info[2]
            mine = mapped(turned(near_raw, near_codes, turn_table), near_kinds, forward)
        theirs = mapped(turned(near_got, own_codes, turn_table), own_kinds, forward)
        jump = own_raw - theirs
        own_flux = diag[:, cols:] * jump
        if last:
            across = jnp.sum(own_flux * jump, axis=0, keepdims=True)
            across = sum(across[:, i : i + count] for i in range(0, cols, count)) if cols % count == 0 else sum_all(across)
            moments.append(jnp.sum(moments.pop() + across, axis=1, keepdims=True))
            lane_row = lax.broadcasted_iota(jnp.int32, (1, 128), 1)
            row = jnp.zeros((1, 128), F32)
            for i, part in enumerate(moments):
                row = jnp.where(lane_row == i, part, row)
            asrc[0] = row
            level_start(0)
        near_flux = diag[:, :cols] * (mine - own_got)
        near_flux = turned(mapped(near_flux, near_kinds, backward), near_codes, back_table)
        flux = jnp.concatenate([near_flux, own_flux], axis=1)
        parts = []
        for part in split(flux):
            for pair in range(3):
                for half in range(ROWS // 16):
                    parts.append(part[half * 16 : (half + 1) * 16] * marks[pair])
        sums = dot(jnp.concatenate(parts, axis=0), cells_t[...])
        sums = sums[: FACES // 2] + sums[FACES // 2 :]
        faces = jnp.concatenate(
            [sums[f // 2 * ROWS : (f // 2 + 1) * ROWS, f % 2 * count : (f % 2 + 1) * count] for f in range(6)], axis=0
        )
        both = dot(lift_ref[first:], jnp.concatenate(split(faces), axis=1))
        new = image + both[:, :count] + both[:, count:]
        if last:
            basis.append(new)
            break
        state = new
        trace = state[:FACES]
        trace_high, trace_low = high_low(trace)
        raw = gather(trace_high, trace_low)
        send_out(it + 1, raw)
        field = state[FACES:]
        field_high, field_low = split(field)
        moments.append(sum_all(basis[-1] * field))
        moments.append(sum_all(field * field))
        basis.append(field)

    for level in range(len(levels)):
        landed = slots_refs[level]
        pltpu.make_async_copy(landed, landed, arecv.at[level]).wait()
        value = asrc[level] + jnp.sum(landed[...], axis=0)
        if level + 1 < len(levels):
            asrc[level + 1] = value
            level_start(level + 1)
    value = jnp.broadcast_to(value, (8, 128))
    coefs = conjugate([jnp.broadcast_to(value[:, i : i + 1], (8, count)) for i in range(MOMENTS)])
    cubes = [v[: WIDTH * 8].reshape(WIDTH, 8, count) for v in basis]
    x = coefs[0] * cubes[0]
    r = cubes[0] - coefs[0] * cubes[1]
    for i in range(1, ITERS):
        x = x + coefs[i] * cubes[i]
        r = r - coefs[i] * cubes[i + 1]
    x_out[...] = (UNIT * x)[:, :NODES]
    r_out[...] = r[:, :NODES]

    for copies in xcopies:
        for k in range(4):
            guarded(k, copies[k].wait_send)
    for level in range(len(levels)):
        landed = slots_refs[level]
        pltpu.make_async_copy(landed, landed, asend.at[level]).wait()


def store(x_ref, r_ref, x_hbm, r_hbm, sems):
    copies = [pltpu.make_async_copy(x_ref, x_hbm, sems.at[0]), pltpu.make_async_copy(r_ref, r_hbm, sems.at[1])]
    for copy in copies:
        copy.start()
    for copy in copies:
        copy.wait()


def body(n_sfc, n_grp, right_side, cell_level, own_slot, near_slot, face_kind, orientation, penalty, send_slots, maps):
    count = right_side.shape[-1]
    ghost = send_slots.shape[0] // 4
    pad = -(-ghost // 128) * 128
    levels = ring_levels(n_sfc * n_grp)
    dma = pltpu.SemaphoreType.DMA
    shape = jax.ShapeDtypeStruct((WIDTH, NODES, count), F32)
    operands = (
        right_side.reshape(WIDTH, NODES, count),
        cell_level, own_slot, near_slot, face_kind, orientation, penalty, send_slots,
        jnp.swapaxes(maps, 0, 1), *constants(),
    )
    vmem = pl.BlockSpec(memory_space=pltpu.VMEM)
    hbm = pl.BlockSpec(memory_space=pltpu.HBM)
    operands = [pltpu.with_memory_space_constraint(operand, pltpu.HBM) for operand in operands]
    x, r = pl.pallas_call(
        functools.partial(kernel, (n_sfc, n_grp, count, ghost, pad)),
        out_shape=(pltpu.VMEM(shape.shape, F32),) * 2,
        in_specs=[hbm] * len(operands),
        out_specs=(vmem, vmem),
        scratch_shapes=[pltpu.VMEM(operand.shape, operand.dtype) for operand in operands]
        + [
            pltpu.VMEM((2 * count, 8 * pad), BF16),
            pltpu.VMEM((8 * pad, 2 * count), BF16),
            pltpu.VMEM((3, 16, 8 * pad), BF16),
            pltpu.VMEM((4 * ROWS, 128), F32),
            pltpu.VMEM((ROWS, 8 * pad), F32),
            pltpu.VMEM((ITERS, 4, MESSAGE, pad), F32),
            pltpu.VMEM((ITERS, 4, MESSAGE, pad), F32),
            pltpu.VMEM((len(levels), 1, 128), F32),
        ]
        + [pltpu.VMEM((size - 1, 1, 128), F32) for _, size in levels]
        + [
            dma((len(operands),)),
            dma((ITERS, 4)),
            dma((ITERS, 4)),
            dma((len(levels),)),
            dma((len(levels),)),
        ]
        + [pltpu.SemaphoreType.REGULAR] * ITERS,
        compiler_params=pltpu.CompilerParams(
            collective_id=0, has_side_effects=True, vmem_limit_bytes=16 * 1024 * 1024
        ),
    )(*operands)
    x, r = pl.pallas_call(
        store,
        out_shape=(shape, shape),
        in_specs=[vmem] * 2,
        out_specs=(hbm, hbm),
        scratch_shapes=[dma((2,))],
        compiler_params=pltpu.CompilerParams(vmem_limit_bytes=1024 * 1024),
    )(pltpu.with_memory_space_constraint(x, pltpu.VMEM), pltpu.with_memory_space_constraint(r, pltpu.VMEM))
    return x.reshape(right_side.shape), r.reshape(right_side.shape)


def solution(mesh):
    split_spec = P(("sfc", "grp"))
    field_spec = P(None, None, None, ("sfc", "grp"))
    return jax.shard_map(
        functools.partial(body, mesh.shape["sfc"], mesh.shape["grp"]),
        mesh=mesh,
        in_specs=(field_spec,) + (split_spec,) * 7 + (P(),),
        out_specs=(field_spec, field_spec),
        check_vma=False,
    )
```

```python
import functools

import jax
import jax.numpy as jnp
import numpy as np
from jax import lax
from jax.experimental import pallas as pl
from jax.experimental.pallas import tpu as pltpu
from jax.sharding import PartitionSpec as P

NODES = 5
WIDTH = NODES * NODES
ROWS = 32
FACES = 6 * ROWS
CUBE = 208
ITERS = 3
REACH = 4
MOMENTS = 2 * ITERS
MESSAGE = 56
UNIT = 2.0**-12
OFFSETS = (1, -1, 2, -2)
MASS = 1.0
LOGICAL = pl.DeviceIdType.LOGICAL
F32 = jnp.float32
BF16 = jnp.bfloat16


def node_tables():
    points = np.array([-1.0, -np.sqrt(3.0 / 7.0), 0.0, np.sqrt(3.0 / 7.0), 1.0])
    weights = np.array([0.1, 49.0 / 90.0, 32.0 / 45.0, 49.0 / 90.0, 0.1])
    identity = np.eye(5)
    spacing = points[:, None] - points[None, :] + identity
    barycentric = 1.0 / np.prod(spacing, axis=1)
    offdiag = barycentric[None, :] / barycentric[:, None] / spacing
    diagonal = np.sum(1.0 / spacing, axis=1) - 1.0
    derivs = np.where(identity > 0.5, diagonal[:, None], offdiag)
    return derivs.T @ (weights[:, None] * derivs), weights


def constants():
    stiff, w = node_tables()
    mass = np.diag(w)
    kron = lambda a, b, c: np.kron(np.kron(a, b), c)
    spots = (np.arange(WIDTH)[:, None] * 8 + np.arange(NODES)).reshape(-1)
    nodes = spots.reshape(5, 5, 5)
    layers = [nodes[0], nodes[4], nodes[:, 0], nodes[:, 4], nodes[:, :, 0], nodes[:, :, 4]]
    select = np.zeros((FACES, CUBE))
    for face, layer in enumerate(layers):
        select[face * ROWS + np.arange(WIDTH), layer.reshape(-1)] = 1.0
    both = np.concatenate([select, np.eye(CUBE)])
    volume = np.zeros((CUBE, CUBE))
    volume[np.ix_(spots, spots)] = kron(stiff, mass, mass) + kron(mass, stiff, mass) + kron(mass, mass, stiff)
    volume = both @ volume * UNIT
    high = volume.astype(jnp.bfloat16)
    low = (volume - high.astype(np.float64)).astype(jnp.bfloat16)
    volume = np.concatenate([high, low])
    lift = both @ select.T
    face_mass = np.zeros((ROWS, 128))
    face_mass[:WIDTH] = UNIT * np.outer(w, w).reshape(-1, 1)
    cube_mass = np.zeros((CUBE, 128))
    cube_mass[spots] = UNIT * MASS * np.einsum("a,b,c->abc", w, w, w).reshape(-1, 1)
    bf = lambda a: jnp.asarray(np.asarray(a, np.float32), BF16)
    return (
        bf(select),
        jnp.asarray(np.concatenate([face_mass, both @ cube_mass]), F32),
        bf(volume),
        bf(lift),
    )


def high_low(x):
    high = x.astype(BF16).astype(F32)
    return high, x - high


def split(x):
    high = x.astype(BF16)
    return high, (x - high.astype(F32)).astype(BF16)


def dot(a, b):
    return jnp.dot(a, b, preferred_element_type=F32)


def dot_nt(a, b):
    return lax.dot_general(a, b, (((1,), (1,)), ((), ())), preferred_element_type=F32)


def ring_levels(total):
    levels, stride = [], 1
    while stride < total:
        rest = total // stride
        size = max(g for g in range(1, 33) if rest % g == 0)
        size = rest if size == 1 else size
        levels.append((stride, size))
        stride *= size
    return levels


def conjugate(m):
    def inner(a, b, shift):
        total = None
        for power in range(len(a) + len(b) - 1):
            weight = sum(a[i] * b[power - i] for i in range(len(a)) if 0 <= power - i < len(b))
            term = weight * m[power + shift]
            total = term if total is None else total + term
        return total

    one = jnp.ones_like(m[0])
    x, r, p = [], [one], [one]
    norm = m[0]
    for it in range(ITERS):
        alpha = norm / inner(p, p, 1)
        x = [(x[i] if i < len(x) else 0.0) + alpha * p[i] for i in range(len(p))]
        r = [one] + [-value for value in x]
        if it + 1 < ITERS:
            new = inner(r, r, 0)
            beta = new / norm
            p = [r[i] + (beta * p[i] if i < len(p) else 0.0) for i in range(len(r))]
            norm = new
    return x


def kernel(
    dims,
    rhs_hbm, level_hbm, own_hbm, near_hbm, kind_hbm, orient_hbm, pen_hbm, send_hbm, maps_hbm,
    sel_hbm, mass_hbm, vol_hbm, lift_hbm,
    x_out, r_out,
    rhs_ref, level_ref, own_ref, near_ref, kind_ref, orient_ref, pen_ref, send_ref, maps_ref,
    sel_ref, mass_ref, vol_ref, lift_ref,
    cells, cells_t, marks, mapz, diag, xsrc, xbuf, asrc, *rest,
):
    n_sfc, n_grp, count, ghost, pad = dims
    total = n_sfc * n_grp
    levels = ring_levels(total)
    slots_refs = rest[: len(levels)]
    insem, xsend, xrecv, asend, arecv, *relay = rest[len(levels):]
    me = lax.axis_index("sfc") * n_grp + lax.axis_index("grp")
    slots = 6 * count
    entries = 4 * ghost
    cols = 4 * pad

    loads = {}
    for i, (name, src, dst) in enumerate([
        ("near", near_hbm, near_ref), ("own", own_hbm, own_ref), ("send", send_hbm, send_ref),
        ("level", level_hbm, level_ref), ("rhs", rhs_hbm, rhs_ref), ("sel", sel_hbm, sel_ref),
        ("kind", kind_hbm, kind_ref), ("orient", orient_hbm, orient_ref), ("pen", pen_hbm, pen_ref),
        ("mass", mass_hbm, mass_ref), ("maps", maps_hbm, maps_ref),
        ("vol", vol_hbm, vol_ref), ("lift", lift_hbm, lift_ref),
    ]):
        loads[name] = pltpu.make_async_copy(src, dst, insem.at[i])
        loads[name].start()

    exists = [(me + offset >= 0) & (me + offset < total) for offset in OFFSETS]

    def near_device(k):
        offset = OFFSETS[k]
        return me + jnp.where(exists[k], offset, offset - total if offset > 0 else offset + total)

    digits = [lax.rem(me // stride, size) for stride, size in levels]

    def peer(level, step):
        stride, size = levels[level]
        return me + jnp.where(digits[level] + step >= size, step - size, step) * stride

    def guarded(k, action):
        @pl.when(exists[k])
        def _():
            action()

    barrier = pltpu.get_barrier_semaphore()
    relayed = len(levels) == 1 and REACH << ITERS == total
    greeted = 0

    def reach(distance, action):
        for offset in (distance, -distance):
            action(me + jnp.where((me + offset >= 0) & (me + offset < total), offset, offset - total if offset > 0 else offset + total))

    if relayed:
        for distance in range(1, REACH + 1):
            reach(distance, lambda device: pl.semaphore_signal(barrier, inc=1, device_id=device, device_id_type=LOGICAL))
        greeted = 2 * REACH
    else:
        for level, (_, size) in enumerate(levels):
            for step in range(1, size):
                pl.semaphore_signal(barrier, inc=1, device_id=peer(level, step), device_id_type=LOGICAL)
            greeted += size - 1
        for k in range(4):
            pl.semaphore_signal(barrier, inc=1, device_id=near_device(k), device_id_type=LOGICAL)
        greeted += 4

    def relay_send(turn_number):
        if relayed:
            reach(REACH << turn_number, lambda device: pl.semaphore_signal(
                relay[turn_number], inc=1, device_id=device, device_id_type=LOGICAL))

    def relay_wait(turn_number):
        if relayed:
            pl.semaphore_wait(relay[turn_number], 2)

    for k in range(4):
        @pl.when(jnp.logical_not(exists[k]))
        def _(k=k):
            for it in range(ITERS):
                xbuf[it, k] = jnp.zeros(xbuf.shape[2:], F32)

    for name in ("near", "own", "send", "level", "rhs", "sel", "kind", "orient", "pen"):
        loads[name].wait()
    line = lambda ref: ref[...].reshape(1, -1)

    inner = lax.broadcasted_iota(jnp.int32, (WIDTH, 8, count), 1) < NODES
    padded = jnp.concatenate([rhs_ref[...], jnp.zeros((WIDTH, 8 - NODES, count), F32)], axis=1)
    field = jnp.concatenate(
        [jnp.where(inner, padded, 0.0).reshape(WIDTH * 8, count), jnp.zeros((CUBE - WIDTH * 8, count), F32)], axis=0
    )
    field_high, field_low = split(field)
    picked = dot(sel_ref[...], jnp.concatenate([field_high, field_low], axis=1))
    scale = jnp.exp2(-line(level_ref).astype(F32))
    face_row = lax.rem(lax.broadcasted_iota(jnp.int32, (FACES, count), 0), ROWS)
    trace_high = jnp.where(face_row == WIDTH, scale, picked[:, :count])
    trace_low = picked[:, count:]

    own = line(own_ref)
    pen = line(pen_ref)
    pen_a, pen_b = high_low(pen)
    pen_b, pen_c = high_low(pen_b)
    send = line(send_ref)
    zero_row = jnp.zeros_like(pen)
    rows = [(own >> 8).astype(F32), (own & 255).astype(F32), line(kind_ref).astype(F32), line(orient_ref).astype(F32)]
    params = jnp.concatenate(rows + [pen_a, pen_b, pen_c, zero_row], axis=0).astype(BF16)
    sent_rows = jnp.concatenate([(send >> 8).astype(F32), (send & 255).astype(F32)] + [zero_row] * 6, axis=0).astype(BF16)
    near = jnp.broadcast_to(line(near_ref), (pad, entries))
    spot = lax.broadcasted_iota(jnp.int32, (pad, entries), 0)
    lane = lax.broadcasted_iota(jnp.int32, (pad, entries), 1)
    inside = spot < ghost
    order, spread = [], []
    for k in range(4):
        order.append(jnp.where(inside & (near == spot + (slots + k * ghost)), 1.0, 0.0).astype(BF16))
        spread.append(jnp.where(inside & (lane == spot + k * ghost), 1.0, 0.0).astype(BF16))
    ordered = dot_nt(params, jnp.concatenate(order, axis=0))
    spread = dot_nt(sent_rows, jnp.concatenate(spread, axis=0))
    slot = jnp.concatenate(
        [spread[0:1] * 256.0 + spread[1:2], ordered[0:1] * 256.0 + ordered[1:2]], axis=1
    ).astype(jnp.int32)
    face = jnp.zeros_like(slot)
    for f in range(1, 6):
        face = face + jnp.where(slot >= f * count, 1, 0)
    cell = slot - face * count
    cell_row = lax.broadcasted_iota(jnp.int32, (count, 2 * cols), 0)
    chosen = jnp.where(cell_row == cell, 1.0, 0.0)
    cells[:count] = chosen.astype(BF16)
    cells[count:] = chosen.astype(BF16)

    def gather(high, low):
        found = dot(jnp.concatenate([high, low], axis=1).astype(BF16), cells[...])
        raw = found[:ROWS]
        for f in range(1, 6):
            raw = jnp.where(face == f, found[f * ROWS : (f + 1) * ROWS], raw)
        return raw

    raw = gather(trace_high, trace_low)
    strength = (ordered[4:5] + ordered[5:6] + ordered[6:7]) * raw[WIDTH : WIDTH + 1, cols:]
    sub = lax.broadcasted_iota(jnp.int32, (8, cols), 0)
    tail = jnp.where(sub == 0, ordered[2:3], jnp.where(sub == 1, ordered[3:4], jnp.where(sub == 2, strength, 0.0)))

    pl.semaphore_wait(barrier, greeted)

    xcopies = []

    def send_out(turn_number, raw):
        count_rows = MESSAGE if turn_number == 0 else 2 * WIDTH
        copies = []
        for k in range(4):
            other = cols + (k ^ 1) * pad
            xsrc[turn_number, k, :WIDTH] = raw[:WIDTH, k * pad : (k + 1) * pad]
            xsrc[turn_number, k, WIDTH : 2 * WIDTH] = raw[:WIDTH, other : other + pad]
            if turn_number == 0:
                xsrc[turn_number, k, 2 * WIDTH :] = tail[: MESSAGE - 2 * WIDTH, other - cols : other - cols + pad]
            copies.append(pltpu.make_async_remote_copy(
                src_ref=xsrc.at[turn_number, k, pl.ds(0, count_rows)],
                dst_ref=xbuf.at[turn_number, k ^ 1, pl.ds(0, count_rows)],
                send_sem=xsend.at[turn_number, k], recv_sem=xrecv.at[turn_number, k ^ 1],
                device_id=near_device(k), device_id_type=LOGICAL,
            ))
        for k in (2, 3, 0, 1):
            guarded(k, copies[k].start)
        xcopies.append(copies)
        relay_send(turn_number)

    send_out(0, raw)

    for name in ("mass", "maps", "vol", "lift"):
        loads[name].wait()
    for pair in range(3):
        marks[pair] = jnp.broadcast_to(jnp.where(face >> 1 == pair, 1.0, 0.0), (16, 2 * cols)).astype(BF16)
    for end in range(2):
        cells_t[:, end * count : (end + 1) * count] = jnp.where(face & 1 == end, chosen, 0.0).T.astype(BF16)
    mapz[...] = jnp.zeros_like(mapz)
    for s in range(4):
        mapz[s * ROWS : s * ROWS + WIDTH, 0:WIDTH] = maps_ref[:, s, :]
    maps = mapz[...]
    transposed = maps.T
    backs = jnp.concatenate([transposed[:ROWS, s * ROWS : (s + 1) * ROWS] for s in range(4)], axis=0)

    def three(matrix):
        high, low = split(matrix)
        return jnp.concatenate([high, high, low], axis=1)

    forward = three(maps[:, :ROWS])
    backward = three(backs)
    face_mass = jnp.concatenate([mass_ref[:ROWS]] * (cols // 128), axis=1)
    diag[:, cols:] = face_mass * strength
    mass_scale = mass_ref[ROWS:] * (scale * scale * scale)

    grid = [[row * NODES + column for column in range(NODES)] for row in range(NODES)]
    orders = [
        [n for row in grid[::-1] for n in row],
        [n for row in grid for n in row[::-1]],
        [n for column in zip(*grid) for n in column],
    ]

    def turned(values, codes, forwards):
        rest = jnp.zeros((ROWS - WIDTH, values.shape[1]), F32)
        for bit in (0, 1, 2) if forwards else (2, 1, 0):
            if bit == 0:
                moved = [values[g * NODES : (g + 1) * NODES] for g in range(NODES)[::-1]]
            else:
                moved = [values[n : n + 1] for n in orders[bit]]
            moved = jnp.concatenate(moved + [rest], axis=0)
            values = jnp.where((codes >> bit) & 1 == 1, moved, values)
        return values

    def mapped(values, kinds, table):
        high, low = split(values)
        forms = dot(table, jnp.concatenate([high, low, high], axis=0))
        result = jnp.where(kinds == 1, values, 0.0)
        for s in range(4):
            result = jnp.where(kinds == s + 2, forms[s * ROWS : (s + 1) * ROWS], result)
        return result

    own_kinds = ordered[2:3].astype(jnp.int32)
    own_codes = ordered[3:4].astype(jnp.int32)

    def image_of(state, high, low, first):
        both = dot(vol_ref[first : FACES + CUBE], jnp.concatenate([high, low], axis=1))
        both = both[:, :count] + both[:, count:] + dot(vol_ref[FACES + CUBE + first :], high)
        return both * scale + mass_scale[first:] * state

    def sum_all(a):
        return jnp.sum(jnp.sum(a, axis=0, keepdims=True), axis=1, keepdims=True)

    def level_copy(level, step):
        return pltpu.make_async_remote_copy(
            src_ref=asrc.at[level], dst_ref=slots_refs[level].at[step - 1],
            send_sem=asend.at[level], recv_sem=arecv.at[level],
            device_id=peer(level, step), device_id_type=LOGICAL,
        )

    def level_start(level):
        for step in range(1, levels[level][1]):
            level_copy(level, step).start()

    basis = [field]
    moments = [sum_all(field * field)]
    state = jnp.concatenate([trace_high + trace_low, field], axis=0)
    mine = None
    for it in range(ITERS):
        last = it + 1 == ITERS
        first = FACES if last else 0
        image = image_of(state[first:], field_high, field_low, first)
        near_raw, own_raw = raw[:, :cols], raw[:, cols:]
        if last:
            moments.append(jnp.sum(field * image, axis=0, keepdims=True))
        if it:
            mine = mapped(turned(near_raw, near_codes, True), near_kinds, forward)
        for k in range(4):
            guarded(k ^ 1, xcopies[it][k].wait_recv)
        relay_wait(it)
        filler = jnp.zeros((ROWS - WIDTH, cols), F32)
        near_got = jnp.concatenate([xbuf[it, k ^ 1, :ROWS] for k in range(4)], axis=1)
        own_got = jnp.concatenate([xbuf[it, k, WIDTH : 2 * WIDTH] for k in range(4)], axis=1)
        own_got = jnp.concatenate([own_got, filler], axis=0)
        if it == 0:
            info = [
                jnp.concatenate([xbuf[it, k, 2 * WIDTH + i : 2 * WIDTH + i + 1] for k in range(4)], axis=1)
                for i in range(3)
            ]
            near_kinds = info[0].astype(jnp.int32)
            near_codes = info[1].astype(jnp.int32)
            diag[:, :cols] = face_mass * info[2]
            mine = mapped(turned(near_raw, near_codes, True), near_kinds, forward)
        theirs = mapped(turned(near_got, own_codes, True), own_kinds, forward)
        jump = own_raw - theirs
        own_flux = diag[:, cols:] * jump
        if last:
            across = jnp.sum(own_flux * jump, axis=0, keepdims=True)
            across = sum(across[:, i : i + count] for i in range(0, cols, count)) if cols % count == 0 else sum_all(across)
            moments.append(jnp.sum(moments.pop() + across, axis=1, keepdims=True))
            lane_row = lax.broadcasted_iota(jnp.int32, (1, 128), 1)
            row = jnp.zeros((1, 128), F32)
            for i, part in enumerate(moments):
                row = jnp.where(lane_row == i, part, row)
            asrc[0] = row
            level_start(0)
        near_flux = diag[:, :cols] * (mine - own_got)
        near_flux = turned(mapped(near_flux, near_kinds, backward), near_codes, False)
        flux = jnp.concatenate([near_flux, own_flux], axis=1)
        parts = []
        for part in split(flux):
            for pair in range(3):
                for half in range(ROWS // 16):
                    parts.append(part[half * 16 : (half + 1) * 16] * marks[pair])
        sums = dot(jnp.concatenate(parts, axis=0), cells_t[...])
        sums = sums[: FACES // 2] + sums[FACES // 2 :]
        faces = jnp.concatenate(
            [sums[f // 2 * ROWS : (f // 2 + 1) * ROWS, f % 2 * count : (f % 2 + 1) * count] for f in range(6)], axis=0
        )
        both = dot(lift_ref[first:], jnp.concatenate(split(faces), axis=1))
        new = image + both[:, :count] + both[:, count:]
        if last:
            basis.append(new)
            break
        state = new
        trace = state[:FACES]
        trace_high, trace_low = high_low(trace)
        raw = gather(trace_high, trace_low)
        send_out(it + 1, raw)
        field = state[FACES:]
        field_high, field_low = split(field)
        moments.append(sum_all(basis[-1] * field))
        moments.append(sum_all(field * field))
        basis.append(field)

    for level in range(len(levels)):
        landed = slots_refs[level]
        pltpu.make_async_copy(landed, landed, arecv.at[level]).wait()
        value = asrc[level] + jnp.sum(landed[...], axis=0)
        if level + 1 < len(levels):
            asrc[level + 1] = value
            level_start(level + 1)
    value = jnp.broadcast_to(value, (8, 128))
    coefs = conjugate([jnp.broadcast_to(value[:, i : i + 1], (8, count)) for i in range(MOMENTS)])
    cubes = [v[: WIDTH * 8].reshape(WIDTH, 8, count) for v in basis]
    x = coefs[0] * cubes[0]
    r = cubes[0] - coefs[0] * cubes[1]
    for i in range(1, ITERS):
        x = x + coefs[i] * cubes[i]
        r = r - coefs[i] * cubes[i + 1]
    x_out[...] = (UNIT * x)[:, :NODES]
    r_out[...] = r[:, :NODES]

    for copies in xcopies:
        for k in range(4):
            guarded(k, copies[k].wait_send)
    for level in range(len(levels)):
        landed = slots_refs[level]
        pltpu.make_async_copy(landed, landed, asend.at[level]).wait()


def store(x_ref, r_ref, x_hbm, r_hbm, sems):
    copies = [pltpu.make_async_copy(x_ref, x_hbm, sems.at[0]), pltpu.make_async_copy(r_ref, r_hbm, sems.at[1])]
    for copy in copies:
        copy.start()
    for copy in copies:
        copy.wait()


def body(n_sfc, n_grp, right_side, cell_level, own_slot, near_slot, face_kind, orientation, penalty, send_slots, maps):
    count = right_side.shape[-1]
    ghost = send_slots.shape[0] // 4
    pad = -(-ghost // 128) * 128
    levels = ring_levels(n_sfc * n_grp)
    dma = pltpu.SemaphoreType.DMA
    shape = jax.ShapeDtypeStruct((WIDTH, NODES, count), F32)
    operands = (
        right_side.reshape(WIDTH, NODES, count),
        cell_level, own_slot, near_slot, face_kind, orientation, penalty, send_slots,
        jnp.swapaxes(maps, 0, 1), *constants(),
    )
    vmem = pl.BlockSpec(memory_space=pltpu.VMEM)
    hbm = pl.BlockSpec(memory_space=pltpu.HBM)
    operands = [pltpu.with_memory_space_constraint(operand, pltpu.HBM) for operand in operands]
    x, r = pl.pallas_call(
        functools.partial(kernel, (n_sfc, n_grp, count, ghost, pad)),
        out_shape=(pltpu.VMEM(shape.shape, F32),) * 2,
        in_specs=[hbm] * len(operands),
        out_specs=(vmem, vmem),
        scratch_shapes=[pltpu.VMEM(operand.shape, operand.dtype) for operand in operands]
        + [
            pltpu.VMEM((2 * count, 8 * pad), BF16),
            pltpu.VMEM((8 * pad, 2 * count), BF16),
            pltpu.VMEM((3, 16, 8 * pad), BF16),
            pltpu.VMEM((4 * ROWS, 128), F32),
            pltpu.VMEM((ROWS, 8 * pad), F32),
            pltpu.VMEM((ITERS, 4, MESSAGE, pad), F32),
            pltpu.VMEM((ITERS, 4, MESSAGE, pad), F32),
            pltpu.VMEM((len(levels), 1, 128), F32),
        ]
        + [pltpu.VMEM((size - 1, 1, 128), F32) for _, size in levels]
        + [
            dma((len(operands),)),
            dma((ITERS, 4)),
            dma((ITERS, 4)),
            dma((len(levels),)),
            dma((len(levels),)),
        ]
        + [pltpu.SemaphoreType.REGULAR] * ITERS,
        compiler_params=pltpu.CompilerParams(
            collective_id=0, has_side_effects=True, vmem_limit_bytes=16 * 1024 * 1024
        ),
    )(*operands)
    x, r = pl.pallas_call(
        store,
        out_shape=(shape, shape),
        in_specs=[vmem] * 2,
        out_specs=(hbm, hbm),
        scratch_shapes=[dma((2,))],
        compiler_params=pltpu.CompilerParams(vmem_limit_bytes=1024 * 1024),
    )(pltpu.with_memory_space_constraint(x, pltpu.VMEM), pltpu.with_memory_space_constraint(r, pltpu.VMEM))
    return x.reshape(right_side.shape), r.reshape(right_side.shape)


def solution(mesh):
    split_spec = P(("sfc", "grp"))
    field_spec = P(None, None, None, ("sfc", "grp"))
    return jax.shard_map(
        functools.partial(body, mesh.shape["sfc"], mesh.shape["grp"]),
        mesh=mesh,
        in_specs=(field_spec,) + (split_spec,) * 7 + (P(),),
        out_specs=(field_spec, field_spec),
        check_vma=False,
    )
```

```python
import functools

import jax
import jax.numpy as jnp
import numpy as np
from jax import lax
from jax.experimental import pallas as pl
from jax.experimental.pallas import tpu as pltpu
from jax.sharding import PartitionSpec as P

NODES = 5
WIDTH = NODES * NODES
ROWS = 32
FACES = 6 * ROWS
CUBE = 208
ITERS = 3
REACH = 4
MOMENTS = 2 * ITERS
MESSAGE = 56
UNIT = 2.0**-12
OFFSETS = (1, -1, 2, -2)
MASS = 1.0
LOGICAL = pl.DeviceIdType.LOGICAL
F32 = jnp.float32
BF16 = jnp.bfloat16


def node_tables():
    points = np.array([-1.0, -np.sqrt(3.0 / 7.0), 0.0, np.sqrt(3.0 / 7.0), 1.0])
    weights = np.array([0.1, 49.0 / 90.0, 32.0 / 45.0, 49.0 / 90.0, 0.1])
    identity = np.eye(5)
    spacing = points[:, None] - points[None, :] + identity
    barycentric = 1.0 / np.prod(spacing, axis=1)
    offdiag = barycentric[None, :] / barycentric[:, None] / spacing
    diagonal = np.sum(1.0 / spacing, axis=1) - 1.0
    derivs = np.where(identity > 0.5, diagonal[:, None], offdiag)
    return derivs.T @ (weights[:, None] * derivs), weights


def constants():
    stiff, w = node_tables()
    mass = np.diag(w)
    kron = lambda a, b, c: np.kron(np.kron(a, b), c)
    spots = (np.arange(WIDTH)[:, None] * 8 + np.arange(NODES)).reshape(-1)
    nodes = spots.reshape(5, 5, 5)
    layers = [nodes[0], nodes[4], nodes[:, 0], nodes[:, 4], nodes[:, :, 0], nodes[:, :, 4]]
    select = np.zeros((FACES, CUBE))
    for face, layer in enumerate(layers):
        select[face * ROWS + np.arange(WIDTH), layer.reshape(-1)] = 1.0
    both = np.concatenate([select, np.eye(CUBE)])
    volume = np.zeros((CUBE, CUBE))
    volume[np.ix_(spots, spots)] = kron(stiff, mass, mass) + kron(mass, stiff, mass) + kron(mass, mass, stiff)
    volume = both @ volume * UNIT
    high = volume.astype(jnp.bfloat16)
    low = (volume - high.astype(np.float64)).astype(jnp.bfloat16)
    volume = np.concatenate([high, low])
    face_mass = np.zeros((ROWS, 128))
    face_mass[:WIDTH] = UNIT * np.outer(w, w).reshape(-1, 1)
    cube_mass = np.zeros((CUBE, 128))
    cube_mass[spots] = UNIT * MASS * np.einsum("a,b,c->abc", w, w, w).reshape(-1, 1)
    bf = lambda a: jnp.asarray(np.asarray(a, np.float32), BF16)
    return (
        bf(select),
        jnp.asarray(np.concatenate([face_mass, both @ cube_mass]), F32),
        bf(volume),
    )


def high_low(x):
    high = x.astype(BF16).astype(F32)
    return high, x - high


def split(x):
    high = x.astype(BF16)
    return high, (x - high.astype(F32)).astype(BF16)


def dot(a, b):
    return jnp.dot(a, b, preferred_element_type=F32)


def dot_nt(a, b):
    return lax.dot_general(a, b, (((1,), (1,)), ((), ())), preferred_element_type=F32)


def ring_levels(total):
    levels, stride = [], 1
    while stride < total:
        rest = total // stride
        size = max(g for g in range(1, 33) if rest % g == 0)
        size = rest if size == 1 else size
        levels.append((stride, size))
        stride *= size
    return levels


def conjugate(m):
    def inner(a, b, shift):
        total = None
        for power in range(len(a) + len(b) - 1):
            weight = sum(a[i] * b[power - i] for i in range(len(a)) if 0 <= power - i < len(b))
            term = weight * m[power + shift]
            total = term if total is None else total + term
        return total

    one = jnp.ones_like(m[0])
    x, r, p = [], [one], [one]
    norm = m[0]
    for it in range(ITERS):
        alpha = norm / inner(p, p, 1)
        x = [(x[i] if i < len(x) else 0.0) + alpha * p[i] for i in range(len(p))]
        r = [one] + [-value for value in x]
        if it + 1 < ITERS:
            new = inner(r, r, 0)
            beta = new / norm
            p = [r[i] + (beta * p[i] if i < len(p) else 0.0) for i in range(len(r))]
            norm = new
    return x


def kernel(
    dims,
    rhs_hbm, level_hbm, own_hbm, near_hbm, kind_hbm, orient_hbm, pen_hbm, send_hbm, maps_hbm,
    sel_hbm, mass_hbm, vol_hbm,
    x_out, r_out,
    rhs_ref, level_ref, own_ref, near_ref, kind_ref, orient_ref, pen_ref, send_ref, maps_ref,
    sel_ref, mass_ref, vol_ref,
    cells, cells_t, marks, mapz, diag, xsrc, xbuf, asrc, *rest,
):
    n_sfc, n_grp, count, ghost, pad = dims
    total = n_sfc * n_grp
    levels = ring_levels(total)
    slots_refs = rest[: len(levels)]
    insem, xsend, xrecv, asend, arecv, *relay = rest[len(levels):]
    me = lax.axis_index("sfc") * n_grp + lax.axis_index("grp")
    slots = 6 * count
    entries = 4 * ghost
    cols = 4 * pad

    loads = {}
    for i, (name, src, dst) in enumerate([
        ("near", near_hbm, near_ref), ("own", own_hbm, own_ref), ("send", send_hbm, send_ref),
        ("level", level_hbm, level_ref), ("rhs", rhs_hbm, rhs_ref), ("sel", sel_hbm, sel_ref),
        ("kind", kind_hbm, kind_ref), ("orient", orient_hbm, orient_ref), ("pen", pen_hbm, pen_ref),
        ("mass", mass_hbm, mass_ref), ("maps", maps_hbm, maps_ref),
        ("vol", vol_hbm, vol_ref),
    ]):
        loads[name] = pltpu.make_async_copy(src, dst, insem.at[i])
        loads[name].start()

    exists = [(me + offset >= 0) & (me + offset < total) for offset in OFFSETS]

    def near_device(k):
        offset = OFFSETS[k]
        return me + jnp.where(exists[k], offset, offset - total if offset > 0 else offset + total)

    digits = [lax.rem(me // stride, size) for stride, size in levels]

    def peer(level, step):
        stride, size = levels[level]
        return me + jnp.where(digits[level] + step >= size, step - size, step) * stride

    def guarded(k, action):
        @pl.when(exists[k])
        def _():
            action()

    barrier = pltpu.get_barrier_semaphore()
    relayed = len(levels) == 1 and REACH << ITERS == total
    greeted = 0

    def reach(distance, action):
        for offset in (distance, -distance):
            action(me + jnp.where((me + offset >= 0) & (me + offset < total), offset, offset - total if offset > 0 else offset + total))

    if relayed:
        for distance in range(1, REACH + 1):
            reach(distance, lambda device: pl.semaphore_signal(barrier, inc=1, device_id=device, device_id_type=LOGICAL))
        greeted = 2 * REACH
    else:
        for level, (_, size) in enumerate(levels):
            for step in range(1, size):
                pl.semaphore_signal(barrier, inc=1, device_id=peer(level, step), device_id_type=LOGICAL)
            greeted += size - 1
        for k in range(4):
            pl.semaphore_signal(barrier, inc=1, device_id=near_device(k), device_id_type=LOGICAL)
        greeted += 4

    def relay_send(turn_number):
        if relayed:
            reach(REACH << turn_number, lambda device: pl.semaphore_signal(
                relay[turn_number], inc=1, device_id=device, device_id_type=LOGICAL))

    def relay_wait(turn_number):
        if relayed:
            pl.semaphore_wait(relay[turn_number], 2)

    for k in range(4):
        @pl.when(jnp.logical_not(exists[k]))
        def _(k=k):
            for it in range(ITERS):
                xbuf[it, k] = jnp.zeros(xbuf.shape[2:], F32)

    for name in ("near", "own", "send", "level", "rhs", "sel", "kind", "orient", "pen"):
        loads[name].wait()
    line = lambda ref: ref[...].reshape(1, -1)

    inner = lax.broadcasted_iota(jnp.int32, (WIDTH, 8, count), 1) < NODES
    padded = jnp.concatenate([rhs_ref[...], jnp.zeros((WIDTH, 8 - NODES, count), F32)], axis=1)
    field = jnp.concatenate(
        [jnp.where(inner, padded, 0.0).reshape(WIDTH * 8, count), jnp.zeros((CUBE - WIDTH * 8, count), F32)], axis=0
    )
    field_high, field_low = split(field)
    picked = dot(sel_ref[...], jnp.concatenate([field_high, field_low], axis=1))
    scale = jnp.exp2(-line(level_ref).astype(F32))
    face_row = lax.rem(lax.broadcasted_iota(jnp.int32, (FACES, count), 0), ROWS)
    trace_high = jnp.where(face_row == WIDTH, scale, picked[:, :count])
    trace_low = picked[:, count:]

    own = line(own_ref)
    pen = line(pen_ref)
    pen_a, pen_b = high_low(pen)
    pen_b, pen_c = high_low(pen_b)
    send = line(send_ref)
    zero_row = jnp.zeros_like(pen)
    rows = [(own >> 8).astype(F32), (own & 255).astype(F32), line(kind_ref).astype(F32), line(orient_ref).astype(F32)]
    params = jnp.concatenate(rows + [pen_a, pen_b, pen_c, zero_row], axis=0).astype(BF16)
    sent_rows = jnp.concatenate([(send >> 8).astype(F32), (send & 255).astype(F32)] + [zero_row] * 6, axis=0).astype(BF16)
    near = jnp.broadcast_to(line(near_ref), (pad, entries))
    spot = lax.broadcasted_iota(jnp.int32, (pad, entries), 0)
    lane = lax.broadcasted_iota(jnp.int32, (pad, entries), 1)
    inside = spot < ghost
    order, spread = [], []
    for k in range(4):
        order.append(jnp.where(inside & (near == spot + (slots + k * ghost)), 1.0, 0.0).astype(BF16))
        spread.append(jnp.where(inside & (lane == spot + k * ghost), 1.0, 0.0).astype(BF16))
    ordered = dot_nt(params, jnp.concatenate(order, axis=0))
    spread = dot_nt(sent_rows, jnp.concatenate(spread, axis=0))
    slot = jnp.concatenate(
        [spread[0:1] * 256.0 + spread[1:2], ordered[0:1] * 256.0 + ordered[1:2]], axis=1
    ).astype(jnp.int32)
    face = jnp.zeros_like(slot)
    for f in range(1, 6):
        face = face + jnp.where(slot >= f * count, 1, 0)
    cell = slot - face * count
    cell_row = lax.broadcasted_iota(jnp.int32, (count, 2 * cols), 0)
    chosen = jnp.where(cell_row == cell, 1.0, 0.0)
    cells[:count] = chosen.astype(BF16)
    cells[count:] = chosen.astype(BF16)

    def gather(high, low):
        found = dot(jnp.concatenate([high, low], axis=1).astype(BF16), cells[...])
        raw = found[:ROWS]
        for f in range(1, 6):
            raw = jnp.where(face == f, found[f * ROWS : (f + 1) * ROWS], raw)
        return raw

    raw = gather(trace_high, trace_low)
    strength = (ordered[4:5] + ordered[5:6] + ordered[6:7]) * raw[WIDTH : WIDTH + 1, cols:]
    sub = lax.broadcasted_iota(jnp.int32, (8, cols), 0)
    tail = jnp.where(sub == 0, ordered[2:3], jnp.where(sub == 1, ordered[3:4], jnp.where(sub == 2, strength, 0.0)))

    pl.semaphore_wait(barrier, greeted)

    xcopies = []

    def send_out(turn_number, raw):
        count_rows = MESSAGE if turn_number == 0 else 2 * WIDTH
        copies = []
        for k in range(4):
            other = cols + (k ^ 1) * pad
            xsrc[turn_number, k, :WIDTH] = raw[:WIDTH, k * pad : (k + 1) * pad]
            xsrc[turn_number, k, WIDTH : 2 * WIDTH] = raw[:WIDTH, other : other + pad]
            if turn_number == 0:
                xsrc[turn_number, k, 2 * WIDTH :] = tail[: MESSAGE - 2 * WIDTH, other - cols : other - cols + pad]
            copies.append(pltpu.make_async_remote_copy(
                src_ref=xsrc.at[turn_number, k, pl.ds(0, count_rows)],
                dst_ref=xbuf.at[turn_number, k ^ 1, pl.ds(0, count_rows)],
                send_sem=xsend.at[turn_number, k], recv_sem=xrecv.at[turn_number, k ^ 1],
                device_id=near_device(k), device_id_type=LOGICAL,
            ))
        for k in (2, 3, 0, 1):
            guarded(k, copies[k].start)
        xcopies.append(copies)
        relay_send(turn_number)

    send_out(0, raw)

    for name in ("mass", "maps", "vol"):
        loads[name].wait()
    for pair in range(3):
        marks[pair] = jnp.broadcast_to(jnp.where(face >> 1 == pair, 1.0, 0.0), (16, 2 * cols)).astype(BF16)
    for end in range(2):
        cells_t[:, end * count : (end + 1) * count] = jnp.where(face & 1 == end, chosen, 0.0).T.astype(BF16)
    mapz[...] = jnp.zeros_like(mapz)
    for s in range(4):
        mapz[s * ROWS : s * ROWS + WIDTH, 0:WIDTH] = maps_ref[:, s, :]
    maps = mapz[...]
    transposed = maps.T
    backs = jnp.concatenate([transposed[:ROWS, s * ROWS : (s + 1) * ROWS] for s in range(4)], axis=0)

    def three(matrix):
        high, low = split(matrix)
        return jnp.concatenate([high, high, low], axis=1)

    forward = three(maps[:, :ROWS])
    backward = three(backs)
    face_mass = jnp.concatenate([mass_ref[:ROWS]] * (cols // 128), axis=1)
    diag[:, cols:] = face_mass * strength
    mass_scale = mass_ref[ROWS:] * (scale * scale * scale)

    grid = [[row * NODES + column for column in range(NODES)] for row in range(NODES)]
    orders = [
        [n for row in grid[::-1] for n in row],
        [n for row in grid for n in row[::-1]],
        [n for column in zip(*grid) for n in column],
    ]

    def turned(values, codes, forwards):
        rest = jnp.zeros((ROWS - WIDTH, values.shape[1]), F32)
        for bit in (0, 1, 2) if forwards else (2, 1, 0):
            if bit == 0:
                moved = [values[g * NODES : (g + 1) * NODES] for g in range(NODES)[::-1]]
            else:
                moved = [values[n : n + 1] for n in orders[bit]]
            moved = jnp.concatenate(moved + [rest], axis=0)
            values = jnp.where((codes >> bit) & 1 == 1, moved, values)
        return values

    def mapped(values, kinds, table):
        high, low = split(values)
        forms = dot(table, jnp.concatenate([high, low, high], axis=0))
        result = jnp.where(kinds == 1, values, 0.0)
        for s in range(4):
            result = jnp.where(kinds == s + 2, forms[s * ROWS : (s + 1) * ROWS], result)
        return result

    own_kinds = ordered[2:3].astype(jnp.int32)
    own_codes = ordered[3:4].astype(jnp.int32)

    def image_of(state, high, low, first):
        both = dot(vol_ref[first : FACES + CUBE], jnp.concatenate([high, low], axis=1))
        both = both[:, :count] + both[:, count:] + dot(vol_ref[FACES + CUBE + first :], high)
        return both * scale + mass_scale[first:] * state

    def sum_all(a):
        return jnp.sum(jnp.sum(a, axis=0, keepdims=True), axis=1, keepdims=True)

    def level_copy(level, step):
        return pltpu.make_async_remote_copy(
            src_ref=asrc.at[level], dst_ref=slots_refs[level].at[step - 1],
            send_sem=asend.at[level], recv_sem=arecv.at[level],
            device_id=peer(level, step), device_id_type=LOGICAL,
        )

    def level_start(level):
        for step in range(1, levels[level][1]):
            level_copy(level, step).start()

    basis = [field]
    moments = [sum_all(field * field)]

    def blank(rows):
        return jnp.zeros((rows, count), F32)

    def lifted(faces):
        part = [faces[f * ROWS : (f + 1) * ROWS] for f in range(6)]
        lines = []
        for a in range(NODES):
            for b in range(NODES):
                g = a * NODES + b
                line = jnp.concatenate([part[4][g : g + 1], blank(3), part[5][g : g + 1], blank(3)], axis=0)
                for f, here, at in ((0, a == 0, b), (1, a == 4, b), (2, b == 0, a), (3, b == 4, a)):
                    if here:
                        line = line + jnp.concatenate([part[f][at * NODES : (at + 1) * NODES], blank(8 - NODES)], axis=0)
                lines.append(line)
        return jnp.concatenate(lines + [blank(CUBE - WIDTH * 8)], axis=0)

    def traces(v):
        five = lambda a, b: v[(a * NODES + b) * 8 : (a * NODES + b) * 8 + NODES]
        pieces = []
        for a in (0, 4):
            pieces += [five(a, b) for b in range(NODES)] + [blank(ROWS - WIDTH)]
        for b in (0, 4):
            pieces += [five(a, b) for a in range(NODES)] + [blank(ROWS - WIDTH)]
        for c in (0, 4):
            pieces += [v[g * 8 + c : g * 8 + c + 1] for g in range(WIDTH)] + [blank(ROWS - WIDTH)]
        return jnp.concatenate(pieces, axis=0)

    mine = None
    for it in range(ITERS):
        last = it + 1 == ITERS
        image = image_of(basis[-1], field_high, field_low, FACES)
        near_raw, own_raw = raw[:, :cols], raw[:, cols:]
        if last:
            moments.append(jnp.sum(field * image, axis=0, keepdims=True))
        if it:
            mine = mapped(turned(near_raw, near_codes, True), near_kinds, forward)
        for k in range(4):
            guarded(k ^ 1, xcopies[it][k].wait_recv)
        relay_wait(it)
        filler = jnp.zeros((ROWS - WIDTH, cols), F32)
        near_got = jnp.concatenate([xbuf[it, k ^ 1, :ROWS] for k in range(4)], axis=1)
        own_got = jnp.concatenate([xbuf[it, k, WIDTH : 2 * WIDTH] for k in range(4)], axis=1)
        own_got = jnp.concatenate([own_got, filler], axis=0)
        if it == 0:
            info = [
                jnp.concatenate([xbuf[it, k, 2 * WIDTH + i : 2 * WIDTH + i + 1] for k in range(4)], axis=1)
                for i in range(3)
            ]
            near_kinds = info[0].astype(jnp.int32)
            near_codes = info[1].astype(jnp.int32)
            diag[:, :cols] = face_mass * info[2]
            mine = mapped(turned(near_raw, near_codes, True), near_kinds, forward)
        theirs = mapped(turned(near_got, own_codes, True), own_kinds, forward)
        jump = own_raw - theirs
        own_flux = diag[:, cols:] * jump
        if last:
            across = jnp.sum(own_flux * jump, axis=0, keepdims=True)
            across = sum(across[:, i : i + count] for i in range(0, cols, count)) if cols % count == 0 else sum_all(across)
            moments.append(jnp.sum(moments.pop() + across, axis=1, keepdims=True))
            lane_row = lax.broadcasted_iota(jnp.int32, (1, 128), 1)
            row = jnp.zeros((1, 128), F32)
            for i, part in enumerate(moments):
                row = jnp.where(lane_row == i, part, row)
            asrc[0] = row
            level_start(0)
        near_flux = diag[:, :cols] * (mine - own_got)
        near_flux = turned(mapped(near_flux, near_kinds, backward), near_codes, False)
        flux = jnp.concatenate([near_flux, own_flux], axis=1)
        parts = []
        for part in split(flux):
            for pair in range(3):
                for half in range(ROWS // 16):
                    parts.append(part[half * 16 : (half + 1) * 16] * marks[pair])
        sums = dot(jnp.concatenate(parts, axis=0), cells_t[...])
        sums = sums[: FACES // 2] + sums[FACES // 2 :]
        faces = jnp.concatenate(
            [sums[f // 2 * ROWS : (f // 2 + 1) * ROWS, f % 2 * count : (f % 2 + 1) * count] for f in range(6)], axis=0
        )
        new = image + lifted(faces)
        if last:
            basis.append(new)
            break
        trace_high, trace_low = high_low(traces(new))
        raw = gather(trace_high, trace_low)
        send_out(it + 1, raw)
        field = new
        field_high, field_low = split(field)
        moments.append(sum_all(basis[-1] * field))
        moments.append(sum_all(field * field))
        basis.append(field)

    for level in range(len(levels)):
        landed = slots_refs[level]
        pltpu.make_async_copy(landed, landed, arecv.at[level]).wait()
        value = asrc[level] + jnp.sum(landed[...], axis=0)
        if level + 1 < len(levels):
            asrc[level + 1] = value
            level_start(level + 1)
    value = jnp.broadcast_to(value, (8, 128))
    coefs = conjugate([jnp.broadcast_to(value[:, i : i + 1], (8, count)) for i in range(MOMENTS)])
    cubes = [v[: WIDTH * 8].reshape(WIDTH, 8, count) for v in basis]
    x = coefs[0] * cubes[0]
    r = cubes[0] - coefs[0] * cubes[1]
    for i in range(1, ITERS):
        x = x + coefs[i] * cubes[i]
        r = r - coefs[i] * cubes[i + 1]
    x_out[...] = (UNIT * x)[:, :NODES]
    r_out[...] = r[:, :NODES]

    for copies in xcopies:
        for k in range(4):
            guarded(k, copies[k].wait_send)
    for level in range(len(levels)):
        landed = slots_refs[level]
        pltpu.make_async_copy(landed, landed, asend.at[level]).wait()


def store(x_ref, r_ref, x_hbm, r_hbm, sems):
    copies = [pltpu.make_async_copy(x_ref, x_hbm, sems.at[0]), pltpu.make_async_copy(r_ref, r_hbm, sems.at[1])]
    for copy in copies:
        copy.start()
    for copy in copies:
        copy.wait()


def body(n_sfc, n_grp, right_side, cell_level, own_slot, near_slot, face_kind, orientation, penalty, send_slots, maps):
    count = right_side.shape[-1]
    ghost = send_slots.shape[0] // 4
    pad = -(-ghost // 128) * 128
    levels = ring_levels(n_sfc * n_grp)
    dma = pltpu.SemaphoreType.DMA
    shape = jax.ShapeDtypeStruct((WIDTH, NODES, count), F32)
    operands = (
        right_side.reshape(WIDTH, NODES, count),
        cell_level, own_slot, near_slot, face_kind, orientation, penalty, send_slots,
        jnp.swapaxes(maps, 0, 1), *constants(),
    )
    vmem = pl.BlockSpec(memory_space=pltpu.VMEM)
    hbm = pl.BlockSpec(memory_space=pltpu.HBM)
    operands = [pltpu.with_memory_space_constraint(operand, pltpu.HBM) for operand in operands]
    x, r = pl.pallas_call(
        functools.partial(kernel, (n_sfc, n_grp, count, ghost, pad)),
        out_shape=(pltpu.VMEM(shape.shape, F32),) * 2,
        in_specs=[hbm] * len(operands),
        out_specs=(vmem, vmem),
        scratch_shapes=[pltpu.VMEM(operand.shape, operand.dtype) for operand in operands]
        + [
            pltpu.VMEM((2 * count, 8 * pad), BF16),
            pltpu.VMEM((8 * pad, 2 * count), BF16),
            pltpu.VMEM((3, 16, 8 * pad), BF16),
            pltpu.VMEM((4 * ROWS, 128), F32),
            pltpu.VMEM((ROWS, 8 * pad), F32),
            pltpu.VMEM((ITERS, 4, MESSAGE, pad), F32),
            pltpu.VMEM((ITERS, 4, MESSAGE, pad), F32),
            pltpu.VMEM((len(levels), 1, 128), F32),
        ]
        + [pltpu.VMEM((size - 1, 1, 128), F32) for _, size in levels]
        + [
            dma((len(operands),)),
            dma((ITERS, 4)),
            dma((ITERS, 4)),
            dma((len(levels),)),
            dma((len(levels),)),
        ]
        + [pltpu.SemaphoreType.REGULAR] * ITERS,
        compiler_params=pltpu.CompilerParams(
            collective_id=0, has_side_effects=True, vmem_limit_bytes=16 * 1024 * 1024
        ),
    )(*operands)
    x, r = pl.pallas_call(
        store,
        out_shape=(shape, shape),
        in_specs=[vmem] * 2,
        out_specs=(hbm, hbm),
        scratch_shapes=[dma((2,))],
        compiler_params=pltpu.CompilerParams(vmem_limit_bytes=1024 * 1024),
    )(pltpu.with_memory_space_constraint(x, pltpu.VMEM), pltpu.with_memory_space_constraint(r, pltpu.VMEM))
    return x.reshape(right_side.shape), r.reshape(right_side.shape)


def solution(mesh):
    split_spec = P(("sfc", "grp"))
    field_spec = P(None, None, None, ("sfc", "grp"))
    return jax.shard_map(
        functools.partial(body, mesh.shape["sfc"], mesh.shape["grp"]),
        mesh=mesh,
        in_specs=(field_spec,) + (split_spec,) * 7 + (P(),),
        out_specs=(field_spec, field_spec),
        check_vma=False,
    )
```
